64 devices in a mesh: data: 4 (over x, y), tensor: 16 (over z, core).
Axes of the slice: x: 2, y: 2, z: 8, core: 2. Of those that a mesh axis runs over, the one named last changes fastest.
The devices are a block of a 4x4x8 slice.
Arguments:
- x: bfloat16 [128, 32, 2560], P('data'), parts along dimension 0
- adapter_ids: int32 [128], P('data'), parts along dimension 0
- norm_gain: float32 [2560], replicated
- w_query: bfloat16 [2560, 32, 80], P(None, 'tensor')
- w_key: bfloat16 [2560, 32, 80], P(None, 'tensor')
- w_value: bfloat16 [2560, 32, 80], P(None, 'tensor')
- w_out: bfloat16 [32, 80, 2560], P('tensor')
- w_gate: bfloat16 [2560, 10240], P(None, 'tensor')
- w_up: bfloat16 [2560, 10240], P(None, 'tensor')
- w_down: bfloat16 [10240, 2560], P('tensor')
- lora_a_query: bfloat16 [4, 2560, 128], P(None, None, 'tensor')
- lora_b_query: bfloat16 [4, 128, 32, 80], P(None, None, 'tensor')
- lora_a_key: bfloat16 [4, 2560, 128], P(None, None, 'tensor')
- lora_b_key: bfloat16 [4, 128, 32, 80], P(None, None, 'tensor')
- lora_a_value: bfloat16 [4, 2560, 128], P(None, None, 'tensor')
- lora_b_value: bfloat16 [4, 128, 32, 80], P(None, None, 'tensor')
- lora_a_out: bfloat16 [4, 32, 80, 128], P(None, 'tensor')
- lora_b_out: bfloat16 [4, 128, 2560], P(None, None, 'tensor')
- lora_a_gate: bfloat16 [4, 2560, 128], P(None, None, 'tensor')
- lora_b_gate: bfloat16 [4, 128, 10240], P(None, None, 'tensor')
- lora_a_up: bfloat16 [4, 2560, 128], P(None, None, 'tensor')
- lora_b_up: bfloat16 [4, 128, 10240], P(None, None, 'tensor')
- lora_a_down: bfloat16 [4, 10240, 128], P(None, 'tensor')
- lora_b_down: bfloat16 [4, 128, 2560], P(None, None, 'tensor')
Outputs:
- output: bfloat16 [128, 32, 2560], P('data'), parts along dimension 0
There are 4 independent parts. The reference program is written for one: setup_inputs(seed, part) draws one part's arguments, and reference() takes and returns one part's arrays. A program takes and returns all parts, laid end to end along the dimension named above; an argument that names none is the same for every part.
All inputs are finite; a program needn't handle non-finite values.
Results may differ from the reference program's by a relative error of at most 0.014501.
Values are sent between devices in bfloat16 or wider.
A program may use at most 768 MiB of HBM per device.

```python
import jax
import jax.numpy as jnp
import math
from jax import lax

SEQS = 32
SEQLEN = 32
D = 2560
HEADS = 32
HEAD = 80
FF = 10240
R = 128
ADAPTERS = 4
ALPHA = 16

EPS = 1e-5
ROPE_BASE = 10000.0
SCALE = ALPHA / R
LORA_FRAC = 0.2


def normal_draw(key, shape, std):
    return (jax.random.normal(key, shape, jnp.float32) * std).astype(jnp.bfloat16)


def setup_inputs(seed: int = 0, part: int = 0) -> dict:
    root = jax.random.key(seed)
    part_key = jax.random.fold_in(root, part)
    x_key, id_key, slot_key = jax.random.split(part_key, 3)
    keys = jax.random.split(root, 22)
    hid_width = HEADS * HEAD
    qk_std = math.log(SEQLEN / 16.0) ** 0.25
    b_std = LORA_FRAC * math.sqrt(R) / ALPHA
    in_std = 1.0 / math.sqrt(D)
    adapter_ids = jax.random.randint(id_key, (SEQS,), 0, ADAPTERS, dtype=jnp.int32)
    slots = jax.random.permutation(slot_key, SEQS)
    adapter_ids = adapter_ids.at[slots[0]].set(ADAPTERS - 1).at[slots[1]].set(0)
    return {
        'x': normal_draw(x_key, (SEQS, SEQLEN, D), 1.0),
        'adapter_ids': adapter_ids,
        'norm_gain': 1.0 + 0.2 * jax.random.normal(keys[0], (D,), jnp.float32),
        'w_query': normal_draw(keys[1], (D, HEADS, HEAD), qk_std * in_std),
        'w_key': normal_draw(keys[2], (D, HEADS, HEAD), qk_std * in_std),
        'w_value': normal_draw(keys[3], (D, HEADS, HEAD), in_std),
        'w_out': normal_draw(keys[4], (HEADS, HEAD, D), 1.0 / math.sqrt(hid_width)),
        'w_gate': normal_draw(keys[5], (D, FF), in_std),
        'w_up': normal_draw(keys[6], (D, FF), in_std),
        'w_down': normal_draw(keys[7], (FF, D), 1.0 / math.sqrt(FF)),
        'lora_a_query': normal_draw(keys[8], (ADAPTERS, D, R), in_std),
        'lora_b_query': normal_draw(keys[9], (ADAPTERS, R, HEADS, HEAD), qk_std * b_std),
        'lora_a_key': normal_draw(keys[10], (ADAPTERS, D, R), in_std),
        'lora_b_key': normal_draw(keys[11], (ADAPTERS, R, HEADS, HEAD), qk_std * b_std),
        'lora_a_value': normal_draw(keys[12], (ADAPTERS, D, R), in_std),
        'lora_b_value': normal_draw(keys[13], (ADAPTERS, R, HEADS, HEAD), b_std),
        'lora_a_out': normal_draw(keys[14], (ADAPTERS, HEADS, HEAD, R), 1.0 / math.sqrt(hid_width)),
        'lora_b_out': normal_draw(keys[15], (ADAPTERS, R, D), b_std),
        'lora_a_gate': normal_draw(keys[16], (ADAPTERS, D, R), in_std),
        'lora_b_gate': normal_draw(keys[17], (ADAPTERS, R, FF), b_std),
        'lora_a_up': normal_draw(keys[18], (ADAPTERS, D, R), in_std),
        'lora_b_up': normal_draw(keys[19], (ADAPTERS, R, FF), b_std),
        'lora_a_down': normal_draw(keys[20], (ADAPTERS, FF, R), 1.0 / math.sqrt(FF)),
        'lora_b_down': normal_draw(keys[21], (ADAPTERS, R, D), b_std),
    }


def rope_rotate(vals, cos_t, sin_t):
    half_dim = vals.shape[-1] // 2
    first = vals[..., :half_dim]
    second = vals[..., half_dim:]
    return jnp.concatenate([first * cos_t - second * sin_t, second * cos_t + first * sin_t], axis=-1)


def lora_proj(rows_in, weight, a_stack, b_stack, adapter):
    base_out = jnp.dot(rows_in, weight, preferred_element_type=jnp.float32)
    lora_mid = jnp.dot(rows_in, a_stack[adapter], preferred_element_type=jnp.float32).astype(jnp.bfloat16)
    return base_out + SCALE * jnp.dot(lora_mid, b_stack[adapter], preferred_element_type=jnp.float32)


def reference(x, adapter_ids, norm_gain, w_query, w_key, w_value, w_out, w_gate, w_up, w_down, lora_a_query, lora_b_query, lora_a_key, lora_b_key, lora_a_value, lora_b_value, lora_a_out, lora_b_out, lora_a_gate, lora_b_gate, lora_a_up, lora_b_up, lora_a_down, lora_b_down):
    hid_width = HEADS * HEAD
    half_dim = HEAD // 2
    inv_freq = ROPE_BASE ** (-jnp.arange(half_dim, dtype=jnp.float32) / half_dim)
    angles = jnp.arange(SEQLEN, dtype=jnp.float32)[:, None] * inv_freq[None, :]
    cos_t = jnp.cos(angles)[:, None, :]
    sin_t = jnp.sin(angles)[:, None, :]
    causal = jnp.arange(SEQLEN)[:, None] >= jnp.arange(SEQLEN)[None, :]
    wq_flat = w_query.reshape(D, hid_width)
    wk_flat = w_key.reshape(D, hid_width)
    wv_flat = w_value.reshape(D, hid_width)
    wo_flat = w_out.reshape(hid_width, D)
    bq_flat = lora_b_query.reshape(ADAPTERS, R, hid_width)
    bk_flat = lora_b_key.reshape(ADAPTERS, R, hid_width)
    bv_flat = lora_b_value.reshape(ADAPTERS, R, hid_width)
    ao_flat = lora_a_out.reshape(ADAPTERS, hid_width, R)

    def one_sequence(seq_item):
        x_seq, adapter = seq_item
        x_f32 = x_seq.astype(jnp.float32)
        normed = (x_f32 * lax.rsqrt(jnp.mean(x_f32 * x_f32, axis=-1, keepdims=True) + EPS) * norm_gain).astype(jnp.bfloat16)
        z_query = lora_proj(normed, wq_flat, lora_a_query, bq_flat, adapter).reshape(SEQLEN, HEADS, HEAD)
        z_key = lora_proj(normed, wk_flat, lora_a_key, bk_flat, adapter).reshape(SEQLEN, HEADS, HEAD)
        z_value = lora_proj(normed, wv_flat, lora_a_value, bv_flat, adapter).reshape(SEQLEN, HEADS, HEAD)
        query_rot = rope_rotate(z_query, cos_t, sin_t).astype(jnp.bfloat16)
        key_rot = rope_rotate(z_key, cos_t, sin_t).astype(jnp.bfloat16)
        value_heads = z_value.astype(jnp.bfloat16)
        scores = jnp.einsum('qhd,khd->hqk', query_rot.astype(jnp.float32), key_rot.astype(jnp.float32)) / math.sqrt(HEAD)
        scores = jnp.where(causal[None], scores, -1e30)
        probs_bf = jax.nn.softmax(scores, axis=-1).astype(jnp.bfloat16)
        attended = jnp.einsum('hqk,khd->qhd', probs_bf.astype(jnp.float32), value_heads.astype(jnp.float32)).astype(jnp.bfloat16).reshape(SEQLEN, hid_width)
        z_out = lora_proj(attended, wo_flat, ao_flat, lora_b_out, adapter)
        gate_pre = lora_proj(normed, w_gate, lora_a_gate, lora_b_gate, adapter)
        up_pre = lora_proj(normed, w_up, lora_a_up, lora_b_up, adapter)
        mlp_mixed = (jax.nn.silu(gate_pre) * up_pre).astype(jnp.bfloat16)
        z_down = lora_proj(mlp_mixed, w_down, lora_a_down, lora_b_down, adapter)
        return (x_f32 + z_out + z_down).astype(jnp.bfloat16)

    return lax.map(one_sequence, (x, adapter_ids))
```

```python
import functools
import math

import jax
import jax.numpy as jnp
import numpy as np
from jax import lax
from jax.experimental import pallas as pl
from jax.experimental.pallas import tpu as pltpu
from jax.sharding import PartitionSpec as P

ALPHA = 16
EPS = 1e-5
ROPE_BASE = 10000.0
MESH = pl.DeviceIdType.MESH
F32 = jnp.float32
BF16 = jnp.bfloat16
PASSES = 2


def mm(lhs, rhs, lc=1, rc=0):
    return lax.dot_general(lhs, rhs, (((lc,), (rc,)), ((), ())), preferred_element_type=F32)


def layer_kernel(cfg, x_hbm, ids_ref, gain_ref, cos_ref, sin_ref,
                 wq, wk, wv, wo, wg, wu, wd,
                 aq, ak, av, ag, au, bq, bk, bv, bg, bu,
                 ao, ad, bo, bd, y_hbm,
                 xv, hv, a_v, wqkv, wgu, bqkv, bgu, wo_v, wd_v, ao_v, ad_v, btg,
                 qkv_base, gu_base, gm, mmk, qk_v, ot_v, m_v, midp,
                 buf, drecv, ring, mg, basef, yv,
                 ld, mid_s, mid_r, md_s, md_r, bt_s, bt_r, dd_s, dd_r, rg_s, rg_r,
                 mg_s, mg_r, ag_s, ag_r, ad_s, ad_r, out_s):
    n, tokens, seq, n_adapt, rank, heads, head, ff = cfg
    chips = n // 2
    half = tokens // PASSES
    wide = heads * head
    share = rank // n
    scale = ALPHA / rank
    d_model = xv.shape[1]
    cols = d_model // (chips // 2)
    rows = half // 4
    mrows = 2 * rank // (chips // 2)
    me = lax.axis_index('tensor')
    chip = me // 2
    core = lax.rem(me, 2)
    sign = 1 - 2 * core
    partner = 2 * chip + 1 - core

    def wrap(c):
        return lax.rem(c + 2 * chips, chips)

    def dev(c):
        return 2 * wrap(c) + core

    def rcopy(src, dst, ssem, rsem, to):
        return pltpu.make_async_remote_copy(src_ref=src, dst_ref=dst, send_sem=ssem, recv_sem=rsem,
                                            device_id={'tensor': to}, device_id_type=MESH)

    loads = []

    def load(src, dst):
        cp = pltpu.make_async_copy(src, dst, ld.at[len(loads)])
        cp.start()
        loads.append(cp)
        return cp

    tile = tokens // 4
    x_ld = [load(x_hbm.at[pl.ds(i * tile, tile)], xv.at[pl.ds(i * tile, tile)]) for i in range(4)]
    a_ld = [load(src, a_v.at[pl.ds(i * n_adapt * share, n_adapt * share)]) for i, src in enumerate((aq, ak, av, ag, au))]

    barrier = pltpu.get_barrier_semaphore()
    for step in range(1, n):
        pl.semaphore_signal(barrier, inc=1, device_id={'tensor': lax.rem(me + step, n)}, device_id_type=MESH)

    w1_ld = [load(src, wqkv.at[pl.ds(i * wide, wide)]) for i, src in enumerate((wq, wk, wv))]
    w2_ld = [load(src, wgu.at[:, pl.ds(i * ff, ff)]) for i, src in enumerate((wg, wu))]

    nt = 128
    for i in range(4):
        x_ld[i].wait()

        def norm_tile(j, carry, i=i):
            r = pl.ds(pl.multiple_of(i * tile + j * nt, nt), nt)
            xf = xv[r, :].astype(F32)
            inv = lax.rsqrt(jnp.mean(xf * xf, axis=-1, keepdims=True) + EPS)
            hv[r, :] = (xf * inv * gain_ref[...]).astype(BF16)
            return carry
        lax.fori_loop(0, tile // nt, norm_tile, 0)

    for cp in a_ld:
        cp.wait()

    def mid_slot(hf, c, k):
        return gm.at[hf, 2 * wrap(c) + k]

    def mid_ring(hf, way, s):
        sg = sign if way == 0 else -sign
        slot = mid_slot(hf, chip - sg * s, core)
        return rcopy(slot, slot, mid_s.at[hf, way, s], mid_r.at[hf, way, s], dev(chip + sg))

    def mid_d2d(hf, i):
        if i == 0:
            c = chip
        elif i <= 4:
            c = chip - sign * i
        else:
            c = chip + sign * (i - 4)
        slot = mid_slot(hf, c, core)
        return rcopy(slot, slot, md_s.at[hf, i], md_r.at[hf, i], partner)

    hch = chips // 2

    def mid_service(hf, s):
        for way in range(2):
            last = hch - way
            if s < last:
                mid_ring(hf, way, s).wait_recv()
                if s + 1 < last:
                    mid_ring(hf, way, s + 1).start()
                mid_d2d(hf, (1 if way == 0 else 5) + s).start()

    def ids_of(start, size):
        return ids_ref[:, pl.ds(start, size)]

    for hf in range(PASSES):
        mids = mm(a_v[...], hv[pl.ds(hf * half, half), :], 1, 1)
        ids = ids_of(hf * half, half)
        out = []
        for st in range(5):
            acc = jnp.zeros((share, half), F32)
            for a in range(n_adapt):
                lo = (st * n_adapt + a) * share
                acc = jnp.where(ids == a, mids[lo:lo + share], acc)
            out.append(acc)
        out.append(jnp.zeros((share, half), F32))
        gm[hf, me] = jnp.concatenate(out, axis=0).astype(BF16)
        if hf == 0:
            pl.semaphore_wait(barrier, n - 1)
        mid_ring(hf, 0, 0).start()
        mid_ring(hf, 1, 0).start()
        mid_d2d(hf, 0).start()

    b_ld = []
    for i, src in enumerate((bq, bk, bv)):
        for a in range(n_adapt):
            b_ld.append(load(src.at[a], bqkv.at[pl.ds(i * wide, wide), pl.ds(a * rank, rank)]))
    b_ld += [load(src, bgu.at[:, pl.ds(i * ff, ff)]) for i, src in enumerate((bg, bu))]
    o_ld = [load(wo, wo_v), load(wd, wd_v)]
    for a in range(n_adapt):
        o_ld.append(load(ao.at[a], ao_v.at[:, pl.ds(a * rank, rank)]))
        o_ld.append(load(ad.at[a], ad_v.at[:, pl.ds(a * rank, rank)]))
    bt_rows = pl.ds(pl.multiple_of(lax.rem(me, 4) * wide, 16), wide)
    bt_ld = []
    for st, src in enumerate((bo, bd)):
        for a in range(n_adapt):
            bt_ld.append(load(src.at[a], btg.at[bt_rows, pl.ds((st * n_adapt + a) * rank, rank)]))

    def base_qkv(hf):
        r = pl.ds(hf * half, half)
        qkv_base[:, r] = mm(wqkv[...], hv[r, :], 1, 1)

    def base_gu(hf, part):
        r = pl.ds(hf * half, half)
        c = pl.ds(part * ff, ff)
        gu_base[r, c] = mm(hv[r, :], wgu[:, c])

    for cp in w1_ld:
        cp.wait()
    base_qkv(0)
    for cp in w2_ld:
        cp.wait()
    base_gu(0, 0)
    mid_service(0, 0)
    mid_service(1, 0)
    base_gu(0, 1)
    base_qkv(1)
    mid_service(0, 1)
    mid_service(1, 1)
    base_gu(1, 0)
    mid_service(0, 2)
    mid_service(1, 2)
    base_gu(1, 1)
    mid_service(0, 3)
    mid_service(1, 3)

    pair = chip + 1 - 2 * lax.rem(chip, 2)

    def bt_slot(dv):
        return btg.at[pl.ds(pl.multiple_of(lax.rem(dv, 4) * wide, 16), wide)]

    bt_out = rcopy(bt_slot(me), bt_slot(me), bt_s.at[0], bt_r.at[0], dev(pair))
    bt_d2d = rcopy(bt_slot(me), bt_slot(me), bt_s.at[1], bt_r.at[1], partner)
    bt_fwd = rcopy(bt_slot(dev(pair)), bt_slot(dev(pair)), bt_s.at[2], bt_r.at[2], partner)
    for cp in bt_ld:
        cp.wait()
    bt_out.start()
    bt_d2d.start()

    for cp in b_ld + o_ld:
        cp.wait()

    def build_mask(hf, st):
        ids = ids_of(hf * half, half)
        parts = [gm[hf, t].astype(F32)[st * share:(st + 1) * share] for t in range(n)]
        full = jnp.concatenate(parts, axis=0)
        for a in range(n_adapt):
            mmk[pl.ds(a * rank, rank), :] = jnp.where(ids == a, full, 0.0).astype(BF16)

    def attend(hf):
        for i in range(8):
            mid_d2d(hf, i).wait_recv()
        r = pl.ds(hf * half, half)
        hd = head // 2
        for st in range(3):
            build_mask(hf, st)
            w = pl.ds(st * wide, wide)
            z = qkv_base[w, r] + scale * mm(bqkv[w, :], mmk[...])
            if st < 2:
                out = []
                for h in range(heads):
                    first = z[h * head:h * head + hd]
                    second = z[h * head + hd:(h + 1) * head]
                    cs, sn = cos_ref[...], sin_ref[...]
                    out += [first * cs - second * sn, second * cs + first * sn]
                z = jnp.concatenate(out, axis=0)
            qk_v[w, :] = z.astype(BF16)
        blk = 256
        qi = lax.broadcasted_iota(jnp.int32, (blk, blk), 0)
        ki = lax.broadcasted_iota(jnp.int32, (blk, blk), 1)
        keep = (qi >= ki) & (qi // seq == ki // seq)
        for h in range(heads):
            for b in range(half // blk):
                c = pl.ds(b * blk, blk)
                qh = qk_v[pl.ds(h * head, head), c]
                kh = qk_v[pl.ds(wide + h * head, head), c]
                vh = qk_v[pl.ds(2 * wide + h * head, head), c]
                sc = mm(qh, kh, 0, 0) * (1.0 / math.sqrt(head))
                sc = jnp.where(keep, sc, -1e30)
                e = jnp.exp(sc - jnp.max(sc, axis=-1, keepdims=True))
                pr = (e * (1.0 / jnp.sum(e, axis=-1, keepdims=True))).astype(BF16)
                ot_v[pl.ds(h * head, head), pl.ds(hf * half + b * blk, blk)] = mm(vh, pr, 1, 1).astype(BF16)

    def pick(full, hf):
        ids = ids_of(hf * half, half)
        acc = jnp.zeros((rank, half), F32)
        for a in range(n_adapt):
            acc = jnp.where(ids == a, full[a * rank:(a + 1) * rank], acc)
        return acc.astype(BF16)

    def gated(hf):
        r = pl.ds(hf * half, half)
        for part in range(2):
            build_mask(hf, 3 + part)
            c = pl.ds(part * ff, ff)
            gu_base[r, c] = gu_base[r, c] + scale * mm(mmk[...], bgu[:, c], 0, 0)
        zg = gu_base[r, pl.ds(0, ff)]
        zu = gu_base[r, pl.ds(ff, ff)]
        m_v[r, :] = (zg / (1.0 + jnp.exp(-zg)) * zu).astype(BF16)
        midp[hf, pl.ds(0, rank), :] = pick(mm(ao_v[...], ot_v[:, r], 0, 0), hf)
        midp[hf, pl.ds(rank, rank), :] = pick(mm(ad_v[...], m_v[r, :], 0, 1), hf)

    def offset_of(i):
        mag = hch - (i + 1) // 2
        return mag * (2 * lax.rem(jnp.int32(i), 2) - 1)

    def d2d(p, i):
        return rcopy(buf.at[p, i, 1 - core], drecv.at[p, i], dd_s.at[p, i], dd_r.at[p, i], partner)

    def piece(p, i):
        e = wrap(chip + offset_of(i))
        odd = lax.rem(e, 2)
        grp = e // 2
        r0 = pl.multiple_of(p * half + odd * 2 * rows, 2 * rows)
        c = pl.ds(pl.multiple_of(grp * cols, 128), cols)
        val = mm(m_v[pl.ds(r0, 2 * rows), :], wd_v[:, c]) + mm(ot_v[:, pl.ds(r0, 2 * rows)], wo_v[:, c], 0, 0)
        for k in range(2):
            buf[p, i, k, pl.ds(0, rows), :] = val[k * rows:(k + 1) * rows].astype(BF16)
            mr = pl.ds(pl.multiple_of(grp * mrows, mrows), mrows)
            mc = pl.ds(pl.multiple_of((odd * 2 + k) * rows, rows), rows)
            blkm = midp[p, mr, mc]
            for b in range(mrows // 16):
                buf[p, i, k, pl.ds(rows, 16), pl.ds(b * rows, rows)] = blkm[b * 16:(b + 1) * 16]
            rest = cols - (mrows // 16) * rows
            buf[p, i, k, pl.ds(rows, 16), pl.ds(cols - rest, rest)] = jnp.zeros((16, rest), BF16)
        d2d(p, i).start()

    def pieces(p, lo, hi):
        def body(i, carry):
            piece(p, i)
            return carry
        lax.fori_loop(lo, hi, body, 0)

    def ring_copy(p, way, s, i):
        sg = sign if way == 0 else -sign
        return rcopy(buf.at[p, i, core], ring.at[p, way, s], rg_s.at[p, way, s], rg_r.at[p, way, s], dev(chip + sg))

    def ring_index(way, s):
        if way == 0:
            return 0 if s == 0 else 2 * s - 1 + core
        return 2 * s + 2 - core

    def ring_step(p, s):
        for way in range(2):
            last = hch - way
            if s >= last:
                continue
            i = ring_index(way, s)
            d2d(p, i).wait_recv()
            tot = buf[p, i, core].astype(F32) + drecv[p, i].astype(F32)
            if s > 0:
                ring_copy(p, way, s - 1, 0).wait_recv()
                tot = tot + ring[p, way, s - 1].astype(F32)
            buf[p, i, core] = tot.astype(BF16)
            ring_copy(p, way, s, i).start()

    def mg_copy(p, d):
        slot = mg.at[p, chip // 2]
        return rcopy(slot, slot, mg_s.at[p, d - 1], mg_r.at[p, d - 1], dev(chip + 2 * d))

    def finish_sum(p):
        i = 2 * hch - 1
        d2d(p, i).wait_recv()
        ring_copy(p, 0, hch - 1, 0).wait_recv()
        ring_copy(p, 1, hch - 2, 0).wait_recv()
        tot = (buf[p, i, core].astype(F32) + drecv[p, i].astype(F32)
               + ring[p, 0, hch - 1].astype(F32) + ring[p, 1, hch - 2].astype(F32))
        basef[p] = tot[:rows]
        tail = tot[rows:]
        for b in range(mrows // 16):
            mg[p, chip // 2, pl.ds(b * 16, 16), :] = tail[:, b * rows:(b + 1) * rows].astype(BF16)
        for d in range(1, hch):
            mg_copy(p, d).start()

    def y_slot(p, c, k):
        c = wrap(c)
        r0 = pl.multiple_of(p * half + (2 * lax.rem(c, 2) + k) * rows, rows)
        return yv.at[pl.ds(r0, rows), pl.ds(pl.multiple_of((c // 2) * cols, 128), cols)]

    def ag_ring(p, way, s):
        sg = sign if way == 0 else -sign
        slot = y_slot(p, chip - sg * s, core)
        return rcopy(slot, slot, ag_s.at[p, way, s], ag_r.at[p, way, s], dev(chip + sg))

    def ag_d2d(p, i):
        if i == 0:
            c = chip
        elif i <= 4:
            c = chip - sign * i
        else:
            c = chip + sign * (i - 4)
        slot = y_slot(p, c, core)
        return rcopy(slot, slot, ad_s.at[p, i], ad_r.at[p, i], partner)

    def ag_service(p, s):
        for way in range(2):
            last = hch - way
            if s < last:
                ag_ring(p, way, s).wait_recv()
                if s + 1 < last:
                    ag_ring(p, way, s + 1).start()
                ag_d2d(p, (1 if way == 0 else 5) + s).start()

    def finish_y(p):
        for d in range(1, hch):
            mg_copy(p, d).wait_recv()
        q = 2 * lax.rem(chip, 2) + core
        t0 = pl.multiple_of(p * half + q * rows, rows)
        c0 = pl.ds(pl.multiple_of((chip // 2) * cols, 128), cols)
        ids = ids_of(t0, rows)
        mids = jnp.concatenate([mg[p, g].astype(F32) for g in range(hch)], axis=0)
        parts = []
        for st in range(2):
            for a in range(n_adapt):
                parts.append(jnp.where(ids == a, mids[st * rank:(st + 1) * rank], 0.0).astype(BF16))
        lora = mm(jnp.concatenate(parts, axis=0), btg[...], 0, 1)
        xs = xv[pl.ds(t0, rows), c0].astype(F32)
        yv[pl.ds(t0, rows), c0] = (xs + basef[p] + scale * lora).astype(BF16)
        ag_ring(p, 0, 0).start()
        ag_ring(p, 1, 0).start()
        ag_d2d(p, 0).start()

    def out_copy(p):
        r = pl.ds(p * half, half)
        return pltpu.make_async_copy(yv.at[r], y_hbm.at[r], out_s.at[p])

    def finish_out(p):
        for i in range(8):
            ag_d2d(p, i).wait_recv()
        out_copy(p).start()

    attend(0)
    gated(0)
    bt_out.wait_recv()
    bt_fwd.start()
    pieces(0, 0, 3)
    ring_step(0, 0)
    pieces(0, 3, 8)
    attend(1)
    ring_step(0, 1)
    gated(1)
    pieces(1, 0, 3)
    ring_step(1, 0)
    ring_step(0, 2)
    pieces(1, 3, 8)
    ring_step(1, 1)
    ring_step(0, 3)
    ring_step(1, 2)
    bt_d2d.wait_recv()
    bt_fwd.wait_recv()
    finish_sum(0)
    ring_step(1, 3)
    finish_y(0)
    finish_sum(1)
    ag_service(0, 0)
    finish_y(1)
    ag_service(0, 1)
    ag_service(1, 0)
    ag_service(0, 2)
    ag_service(1, 1)
    ag_service(0, 3)
    ag_service(1, 2)
    finish_out(0)
    ag_service(1, 3)
    finish_out(1)

    for p in range(PASSES):
        for i in range(8):
            mid_d2d(p, i).wait_send()
            d2d(p, i).wait_send()
            ag_d2d(p, i).wait_send()
        for way in range(2):
            for s in range(hch - way):
                mid_ring(p, way, s).wait_send()
                ring_copy(p, way, s, 0).wait_send()
                ag_ring(p, way, s).wait_send()
        for d in range(1, hch):
            mg_copy(p, d).wait_send()
        out_copy(p).wait()
    bt_out.wait_send()
    bt_d2d.wait_send()
    bt_fwd.wait_send()


def solution(mesh):
    n = mesh.shape['tensor']
    batch_spec = P('data', None, None)
    head_cols = P(None, 'tensor', None)
    head_rows = P('tensor', None, None)
    ff_cols = P(None, 'tensor')
    ff_rows = P('tensor', None)
    last_split = P(None, None, 'tensor')
    b_heads = P(None, None, 'tensor', None)
    a_heads = P(None, 'tensor', None, None)
    in_specs = (batch_spec, P('data'), P(None), head_cols, head_cols, head_cols, head_rows, ff_cols, ff_cols, ff_rows, last_split, b_heads, last_split, b_heads, last_split, b_heads, a_heads, last_split, last_split, last_split, last_split, last_split, head_cols, last_split)

    def local_layer(x_blk, adapter_ids, norm_gain, w_query, w_key, w_value, w_out, w_gate, w_up, w_down, a_query, b_query, a_key, b_key, a_value, b_value, a_out, b_out, a_gate, b_gate, a_up, b_up, a_down, b_down):
        seqs, seq, d_model = x_blk.shape
        tokens = seqs * seq
        n_adapt, _, rank = a_down.shape
        heads, head = w_query.shape[1:]
        wide = heads * head
        ff = w_gate.shape[1]
        chips = n // 2
        half = tokens // PASSES
        rows = half // 4
        cols = d_model // (chips // 2)
        mrows = 2 * rank // (chips // 2)
        share = rank // n

        ids = jnp.repeat(adapter_ids, seq).reshape(1, tokens)
        hd = head // 2
        inv_freq = ROPE_BASE ** (-np.arange(hd, dtype=np.float32) / np.float32(hd))
        ang = inv_freq[:, None] * np.arange(seq, dtype=np.float32)[None, :]
        ang = np.tile(ang.astype(np.float32), (1, half // seq))
        cos_t, sin_t = jnp.asarray(np.cos(ang), F32), jnp.asarray(np.sin(ang), F32)

        def wt(w):
            return w.transpose(1, 2, 0).reshape(wide, d_model)

        def at(a):
            return a.transpose(0, 2, 1).reshape(n_adapt * share, d_model)

        def bt(b):
            return b.transpose(0, 2, 3, 1).reshape(n_adapt, wide, rank)

        args = (x_blk.reshape(tokens, d_model), ids, norm_gain.reshape(1, d_model), cos_t, sin_t,
                wt(w_query), wt(w_key), wt(w_value), w_out.reshape(wide, d_model), w_gate, w_up, w_down,
                at(a_query), at(a_key), at(a_value), at(a_gate), at(a_up),
                bt(b_query), bt(b_key), bt(b_value), b_gate.reshape(n_adapt * rank, ff), b_up.reshape(n_adapt * rank, ff),
                a_out.reshape(n_adapt, wide, rank), a_down, b_out.transpose(0, 2, 1), b_down.transpose(0, 2, 1))
        hbm = pl.BlockSpec(memory_space=pl.ANY)
        vmem = pl.BlockSpec(memory_space=pltpu.VMEM)
        dma = pltpu.SemaphoreType.DMA
        cfg = (n, tokens, seq, n_adapt, rank, heads, head, ff)
        scratch = [
            pltpu.VMEM((tokens, d_model), BF16),
            pltpu.VMEM((tokens, d_model), BF16),
            pltpu.VMEM((5 * n_adapt * share, d_model), BF16),
            pltpu.VMEM((3 * wide, d_model), BF16),
            pltpu.VMEM((d_model, 2 * ff), BF16),
            pltpu.VMEM((3 * wide, n_adapt * rank), BF16),
            pltpu.VMEM((n_adapt * rank, 2 * ff), BF16),
            pltpu.VMEM((wide, d_model), BF16),
            pltpu.VMEM((ff, d_model), BF16),
            pltpu.VMEM((wide, n_adapt * rank), BF16),
            pltpu.VMEM((ff, n_adapt * rank), BF16),
            pltpu.VMEM((4 * wide, 2 * n_adapt * rank), BF16),
            pltpu.VMEM((3 * wide, tokens), F32),
            pltpu.VMEM((tokens, 2 * ff), F32),
            pltpu.VMEM((PASSES, n, 6 * share, half), BF16),
            pltpu.VMEM((n_adapt * rank, half), BF16),
            pltpu.VMEM((3 * wide, half), BF16),
            pltpu.VMEM((wide, tokens), BF16),
            pltpu.VMEM((tokens, ff), BF16),
            pltpu.VMEM((PASSES, 2 * rank, half), BF16),
            pltpu.VMEM((PASSES, chips, 2, rows + 16, cols), BF16),
            pltpu.VMEM((PASSES, chips, rows + 16, cols), BF16),
            pltpu.VMEM((PASSES, 2, chips // 2, rows + 16, cols), BF16),
            pltpu.VMEM((PASSES, chips // 2, mrows, rows), BF16),
            pltpu.VMEM((PASSES, rows, cols), F32),
            pltpu.VMEM((tokens, d_model), BF16),
            dma((48,)),
            dma((PASSES, 2, 4)), dma((PASSES, 2, 4)), dma((PASSES, 8)), dma((PASSES, 8)),
            dma((3,)), dma((3,)), dma((PASSES, 8)), dma((PASSES, 8)),
            dma((PASSES, 2, 4)), dma((PASSES, 2, 4)), dma((PASSES, 3)), dma((PASSES, 3)),
            dma((PASSES, 2, 4)), dma((PASSES, 2, 4)), dma((PASSES, 8)), dma((PASSES, 8)),
            dma((PASSES,)),
        ]
        y = pl.pallas_call(
            functools.partial(layer_kernel, cfg),
            out_shape=jax.ShapeDtypeStruct((tokens, d_model), BF16),
            in_specs=[hbm] + [vmem] * 4 + [hbm] * 21,
            out_specs=hbm,
            scratch_shapes=scratch,
            compiler_params=pltpu.CompilerParams(collective_id=0, has_side_effects=True,
                                                 vmem_limit_bytes=67_000_000),
        )(*args)
        return y.reshape(x_blk.shape)

    return jax.shard_map(local_layer, mesh=mesh, in_specs=in_specs, out_specs=batch_spec, check_vma=False)
```

```python
import functools
import math

import jax
import jax.numpy as jnp
import numpy as np
from jax import lax
from jax.experimental import pallas as pl
from jax.experimental.pallas import tpu as pltpu
from jax.sharding import PartitionSpec as P

ALPHA = 16
EPS = 1e-5
ROPE_BASE = 10000.0
MESH = pl.DeviceIdType.MESH
F32 = jnp.float32
BF16 = jnp.bfloat16
PASSES = 2
SUBS = 2


def mm(lhs, rhs, lc=1, rc=0):
    return lax.dot_general(lhs, rhs, (((lc,), (rc,)), ((), ())), preferred_element_type=F32)


def layer_kernel(cfg, x_hbm, ids_hbm, gain_hbm, cos_hbm, sin_hbm,
                 wq, wk, wv, wo, wg, wu, wd,
                 aq, ak, av, ag, au, bq, bk, bv, bg, bu,
                 ao, ad, bo, bd, yv,
                 ids_s, ids_ref, gain_v, gain_ref, cos_ref, sin_ref, xv, hv, a_v, wqkv, wgu, bqkv, bgu, wo_v, wd_v, ao_v, ad_v, btg,
                 qkv_base, gu_base, gm, mmk, qk_v, ot_v, m_v, midp, midr, midx,
                 buf, drecv, ring, mg, xo,
                 ld, mid_s, mid_r, md_s, md_r, bt_s, bt_r, dd_s, dd_r, rg_s, rg_r,
                 mp_s, mp_r, mx_s, mx_r, mg_s, mg_r, ag_s, ag_r, ad_s, ad_r):
    n, tokens, seq, n_adapt, rank, heads, head, ff = cfg
    chips = n // 2
    half = tokens // PASSES
    wide = heads * head
    share = rank // n
    scale = ALPHA / rank
    d_model = xv.shape[1]
    cols = d_model // (chips // 2)
    rows = half // 4
    mrows = 2 * rank // (chips // 2)
    me = lax.axis_index('tensor')
    chip = me // 2
    core = lax.rem(me, 2)
    sign = 1 - 2 * core
    partner = 2 * chip + 1 - core

    def wrap(c):
        return lax.rem(c + 2 * chips, chips)

    def dev(c):
        return 2 * wrap(c) + core

    def rcopy(src, dst, ssem, rsem, to):
        return pltpu.make_async_remote_copy(src_ref=src, dst_ref=dst, send_sem=ssem, recv_sem=rsem,
                                            device_id={'tensor': to}, device_id_type=MESH)

    loads = []

    def load(src, dst):
        cp = pltpu.make_async_copy(src, dst, ld.at[len(loads)])
        cp.start()
        loads.append(cp)
        return cp

    tile = tokens // 4
    g_ld = [load(ids_hbm, ids_s), load(gain_hbm, gain_v)]
    x_ld = [load(x_hbm.at[pl.ds(i * tile, tile)], xv.at[pl.ds(i * tile, tile)]) for i in range(4)]
    a_ld = [load(src, a_v.at[pl.ds(i * n_adapt * share, n_adapt * share)]) for i, src in enumerate((aq, ak, av, ag, au))]

    barrier = pltpu.get_barrier_semaphore()
    for step in range(1, n):
        pl.semaphore_signal(barrier, inc=1, device_id={'tensor': lax.rem(me + step, n)}, device_id_type=MESH)

    w1_ld = [load(src, wqkv.at[pl.ds(i * wide, wide)]) for i, src in enumerate((wq, wk, wv))]
    w2_ld = [load(src, wgu.at[:, pl.ds(i * ff, ff)]) for i, src in enumerate((wg, wu))]

    c_ld = [load(cos_hbm, cos_ref), load(sin_hbm, sin_ref)]
    for cp in g_ld:
        cp.wait()
    where_seq = lax.broadcasted_iota(jnp.int32, (1, tokens), 1) // seq
    ids_all = jnp.zeros((1, tokens), jnp.int32)
    for b in range(tokens // seq):
        ids_all = jnp.where(where_seq == b, ids_s[b], ids_all)
    ids_ref[...] = ids_all
    gain_ref[...] = jnp.concatenate([gain_v[b:b + 1, :] for b in range(gain_v.shape[0])], axis=1)

    nt = 128
    for i in range(4):
        x_ld[i].wait()

        def norm_tile(j, carry, i=i):
            r = pl.ds(pl.multiple_of(i * tile + j * nt, nt), nt)
            xf = xv[r, :].astype(F32)
            inv = lax.rsqrt(jnp.mean(xf * xf, axis=-1, keepdims=True) + EPS)
            hv[r, :] = (xf * inv * gain_ref[...]).astype(BF16)
            return carry
        lax.fori_loop(0, tile // nt, norm_tile, 0)

    for cp in a_ld:
        cp.wait()

    def mid_slot(hf, c, k):
        return gm.at[hf, 2 * wrap(c) + k]

    def mid_ring(hf, way, s):
        sg = sign if way == 0 else -sign
        slot = mid_slot(hf, chip - sg * s, core)
        return rcopy(slot, slot, mid_s.at[hf, way, s], mid_r.at[hf, way, s], dev(chip + sg))

    def mid_d2d(hf, i):
        if i == 0:
            c = chip
        elif i <= 4:
            c = chip - sign * i
        else:
            c = chip + sign * (i - 4)
        slot = mid_slot(hf, c, core)
        return rcopy(slot, slot, md_s.at[hf, i], md_r.at[hf, i], partner)

    hch = chips // 2

    def mid_service(hf, s):
        for way in range(2):
            last = hch - way
            if s < last:
                mid_ring(hf, way, s).wait_recv()
                if s + 1 < last:
                    mid_ring(hf, way, s + 1).start()
                mid_d2d(hf, (1 if way == 0 else 5) + s).start()

    def ids_of(start, size):
        return ids_ref[:, pl.ds(start, size)]

    for hf in range(PASSES):
        mids = mm(a_v[...], hv[pl.ds(hf * half, half), :], 1, 1)
        ids = ids_of(hf * half, half)
        out = []
        for st in range(5):
            acc = jnp.zeros((share, half), F32)
            for a in range(n_adapt):
                lo = (st * n_adapt + a) * share
                acc = jnp.where(ids == a, mids[lo:lo + share], acc)
            out.append(acc)
        out.append(jnp.zeros((share, half), F32))
        gm[hf, me] = jnp.concatenate(out, axis=0).astype(BF16)
        if hf == 0:
            pl.semaphore_wait(barrier, n - 1)
        mid_ring(hf, 0, 0).start()
        mid_ring(hf, 1, 0).start()
        mid_d2d(hf, 0).start()

    b_ld = []
    for i, src in enumerate((bq, bk, bv)):
        for a in range(n_adapt):
            b_ld.append(load(src.at[a], bqkv.at[pl.ds(i * wide, wide), pl.ds(a * rank, rank)]))
    b_ld += [load(src, bgu.at[:, pl.ds(i * ff, ff)]) for i, src in enumerate((bg, bu))]
    o_ld = [load(wo, wo_v), load(wd, wd_v)]
    for a in range(n_adapt):
        o_ld.append(load(ao.at[a], ao_v.at[:, pl.ds(a * rank, rank)]))
        o_ld.append(load(ad.at[a], ad_v.at[:, pl.ds(a * rank, rank)]))
    bt_rows = pl.ds(pl.multiple_of(lax.rem(me, 4) * wide, 16), wide)
    bt_ld = []
    for st, src in enumerate((bo, bd)):
        for a in range(n_adapt):
            bt_ld.append(load(src.at[a], btg.at[bt_rows, pl.ds((st * n_adapt + a) * rank, rank)]))

    def base_qkv(hf):
        r = pl.ds(hf * half, half)
        qkv_base[:, r] = mm(wqkv[...], hv[r, :], 1, 1)

    def base_gu(hf, part):
        r = pl.ds(hf * half, half)
        c = pl.ds(part * ff, ff)
        gu_base[r, c] = mm(hv[r, :], wgu[:, c])

    pair = chip + 1 - 2 * lax.rem(chip, 2)

    def bt_slot(dv):
        return btg.at[pl.ds(pl.multiple_of(lax.rem(dv, 4) * wide, 16), wide)]

    bt_out = rcopy(bt_slot(me), bt_slot(me), bt_s.at[0], bt_r.at[0], dev(pair))
    bt_d2d = rcopy(bt_slot(me), bt_slot(me), bt_s.at[1], bt_r.at[1], partner)
    bt_fwd = rcopy(bt_slot(dev(pair)), bt_slot(dev(pair)), bt_s.at[2], bt_r.at[2], partner)
    def build_mask(hf, st):
        ids = ids_of(hf * half, half)
        parts = [gm[hf, t].astype(F32)[st * share:(st + 1) * share] for t in range(n)]
        full = jnp.concatenate(parts, axis=0)
        for a in range(n_adapt):
            mmk[pl.ds(a * rank, rank), :] = jnp.where(ids == a, full, 0.0).astype(BF16)

    def attend(hf):
        for i in range(8):
            mid_d2d(hf, i).wait_recv()
        r = pl.ds(hf * half, half)
        hd = head // 2
        for st in range(3):
            build_mask(hf, st)
            w = pl.ds(st * wide, wide)
            z = qkv_base[w, r] + scale * mm(bqkv[w, :], mmk[...])
            if st < 2:
                out = []
                for h in range(heads):
                    first = z[h * head:h * head + hd]
                    second = z[h * head + hd:(h + 1) * head]
                    cs, sn = cos_ref[...], sin_ref[...]
                    out += [first * cs - second * sn, second * cs + first * sn]
                z = jnp.concatenate(out, axis=0)
            qk_v[w, :] = z.astype(BF16)
        blk = 256
        qi = lax.broadcasted_iota(jnp.int32, (blk, blk), 0)
        ki = lax.broadcasted_iota(jnp.int32, (blk, blk), 1)
        keep = (qi >= ki) & (qi // seq == ki // seq)
        for h in range(heads):
            for b in range(half // blk):
                c = pl.ds(b * blk, blk)
                qh = qk_v[pl.ds(h * head, head), c]
                kh = qk_v[pl.ds(wide + h * head, head), c]
                vh = qk_v[pl.ds(2 * wide + h * head, head), c]
                sc = mm(qh, kh, 0, 0) * (1.0 / math.sqrt(head))
                sc = jnp.where(keep, sc, -1e30)
                e = jnp.exp(sc - jnp.max(sc, axis=-1, keepdims=True))
                pr = (e * (1.0 / jnp.sum(e, axis=-1, keepdims=True))).astype(BF16)
                ot_v[pl.ds(h * head, head), pl.ds(hf * half + b * blk, blk)] = mm(vh, pr, 1, 1).astype(BF16)

    def pick(full, hf):
        ids = ids_of(hf * half, half)
        acc = jnp.zeros((rank, half), F32)
        for a in range(n_adapt):
            acc = jnp.where(ids == a, full[a * rank:(a + 1) * rank], acc)
        return acc.astype(BF16)

    def gated(hf):
        r = pl.ds(hf * half, half)
        for part in range(2):
            build_mask(hf, 3 + part)
            c = pl.ds(part * ff, ff)
            gu_base[r, c] = gu_base[r, c] + scale * mm(mmk[...], bgu[:, c], 0, 0)
        zg = gu_base[r, pl.ds(0, ff)]
        zu = gu_base[r, pl.ds(ff, ff)]
        m_v[r, :] = (zg / (1.0 + jnp.exp(-zg)) * zu).astype(BF16)
        for st, acc in enumerate((pick(mm(ao_v[...], ot_v[:, r], 0, 0), hf), pick(mm(ad_v[...], m_v[r, :], 0, 1), hf))):
            for q in range(4):
                midp[hf, q % 2, q // 2, pl.ds(st * rank, rank), :] = acc[:, q * rows:(q + 1) * rows]
        mid_part(hf).start()

    def mid_part(p):
        return rcopy(midp.at[p, 1 - core], midr.at[p], mp_s.at[p], mp_r.at[p], partner)

    def mid_block(p, c):
        c = wrap(c)
        return midp.at[p, core, lax.rem(c, 2), pl.ds(pl.multiple_of((c // 2) * mrows, mrows), mrows)]

    def mid_send(p, d):
        return rcopy(mid_block(p, chip + d), midx.at[p, d - 1], mx_s.at[p, d - 1], mx_r.at[p, d - 1], dev(chip + d))

    def mid_scatter(p):
        mid_part(p).wait_recv()
        midp[p, core] = (midp[p, core].astype(F32) + midr[p].astype(F32)).astype(BF16)
        for d in (4, 3, 5, 2, 6, 1, 7):
            mid_send(p, d).start()

    def mid_gather(p):
        tot = mid_block(p, chip)[...].astype(F32)
        for d in range(1, chips):
            mid_send(p, d).wait_recv()
            tot = tot + midx[p, d - 1].astype(F32)
        mg[p, chip // 2] = tot.astype(BF16)
        for d in range(1, hch):
            mg_copy(p, d).start()

    def offset_of(i):
        mag = hch - (i + 1) // 2
        return mag * (2 * lax.rem(jnp.int32(i), 2) - 1)

    def d2d(p, i):
        return rcopy(buf.at[p, i, 1 - core], drecv.at[p, i], dd_s.at[p, i], dd_r.at[p, i], partner)

    def piece(p, i):
        e = wrap(chip + offset_of(i))
        odd = lax.rem(e, 2)
        grp = e // 2
        r0 = pl.multiple_of(p * half + odd * 2 * rows, 2 * rows)
        c = pl.ds(pl.multiple_of(grp * cols, 128), cols)
        val = mm(m_v[pl.ds(r0, 2 * rows), :], wd_v[:, c]) + mm(ot_v[:, pl.ds(r0, 2 * rows)], wo_v[:, c], 0, 0)
        for k in range(2):
            buf[p, i, k] = val[k * rows:(k + 1) * rows].astype(BF16)
        d2d(p, i).start()

    def pieces(p, lo, hi):
        def body(i, carry):
            piece(p, i)
            return carry
        lax.fori_loop(lo, hi, body, 0)

    def sub(u):
        return pl.ds(u * (rows // SUBS), rows // SUBS)

    def ring_copy(p, way, s, u, i):
        sg = sign if way == 0 else -sign
        return rcopy(buf.at[p, i, core, sub(u)], ring.at[p, way, s, sub(u)],
                     rg_s.at[p, way, s, u], rg_r.at[p, way, s, u], dev(chip + sg))

    def ring_index(way, s):
        if way == 0:
            return 0 if s == 0 else 2 * s - 1 + core
        return 2 * s + 2 - core

    def ring_step(p, s):
        for u in range(SUBS):
            for way in range(2):
                last = hch - way
                if s >= last:
                    continue
                i = ring_index(way, s)
                if u == 0:
                    d2d(p, i).wait_recv()
                tot = buf[p, i, core, sub(u)].astype(F32) + drecv[p, i, sub(u)].astype(F32)
                if s > 0:
                    ring_copy(p, way, s - 1, u, 0).wait_recv()
                    tot = tot + ring[p, way, s - 1, sub(u)].astype(F32)
                buf[p, i, core, sub(u)] = tot.astype(BF16)
                ring_copy(p, way, s, u, i).start()

    def mg_copy(p, d):
        slot = mg.at[p, chip // 2]
        return rcopy(slot, slot, mg_s.at[p, d - 1], mg_r.at[p, d - 1], dev(chip + 2 * d))

    def y_rows(p, c, k, u):
        c = wrap(c)
        return pl.multiple_of(p * half + (2 * lax.rem(c, 2) + k) * rows + u * (rows // SUBS), rows // SUBS)

    def y_cols(c):
        return pl.ds(pl.multiple_of((wrap(c) // 2) * cols, 128), cols)

    def y_slot(p, c, k, u):
        return yv.at[pl.ds(y_rows(p, c, k, u), rows // SUBS), y_cols(c)]

    def ag_ring(p, way, s, u):
        sg = sign if way == 0 else -sign
        slot = y_slot(p, chip - sg * s, core, u)
        return rcopy(slot, slot, ag_s.at[p, way, s, u], ag_r.at[p, way, s, u], dev(chip + sg))

    def ag_d2d(p, i, u):
        if i == 0:
            c = chip
        elif i <= 4:
            c = chip - sign * i
        else:
            c = chip + sign * (i - 4)
        slot = y_slot(p, c, core, u)
        return rcopy(slot, slot, ad_s.at[p, i, u], ad_r.at[p, i, u], partner)

    def ag_service(p, s):
        for u in range(SUBS):
            for way in range(2):
                last = hch - way
                if s < last:
                    ag_ring(p, way, s, u).wait_recv()
                    if s + 1 < last:
                        ag_ring(p, way, s + 1, u).start()
                    ag_d2d(p, (1 if way == 0 else 5) + s, u).start()

    def lora_out(p):
        for d in range(1, hch):
            mg_copy(p, d).wait_recv()
        ids = ids_of(y_rows(p, chip, core, 0), rows)
        mids = jnp.concatenate([mg[p, g].astype(F32) for g in range(hch)], axis=0)
        parts = []
        for st in range(2):
            for a in range(n_adapt):
                parts.append(jnp.where(ids == a, mids[st * rank:(st + 1) * rank], 0.0).astype(BF16))
        lora = mm(jnp.concatenate(parts, axis=0), btg[...], 0, 1)
        r = pl.ds(y_rows(p, chip, core, 0), rows)
        xo[p] = xv[r, y_cols(chip)].astype(F32) + scale * lora

    def finish_y(p):
        i = 2 * hch - 1
        d2d(p, i).wait_recv()
        for u in range(SUBS):
            tot = buf[p, i, core, sub(u)].astype(F32) + drecv[p, i, sub(u)].astype(F32)
            for way in range(2):
                ring_copy(p, way, hch - 1 - way, u, 0).wait_recv()
                tot = tot + ring[p, way, hch - 1 - way, sub(u)].astype(F32)
            y_slot(p, chip, core, u)[...] = (xo[p, sub(u)] + tot).astype(BF16)
            ag_ring(p, 0, 0, u).start()
            ag_ring(p, 1, 0, u).start()
            ag_d2d(p, 0, u).start()

    for cp in w1_ld:
        cp.wait()
    base_qkv(0)
    for cp in w2_ld:
        cp.wait()
    base_gu(0, 0)
    mid_service(0, 0)
    base_gu(0, 1)
    mid_service(1, 0)
    mid_service(0, 1)
    base_qkv(1)
    mid_service(1, 1)
    mid_service(0, 2)
    base_gu(1, 0)
    mid_service(1, 2)
    mid_service(0, 3)
    for cp in c_ld + b_ld + o_ld + bt_ld:
        cp.wait()
    attend(0)
    mid_service(1, 3)
    bt_out.start()
    bt_d2d.start()
    gated(0)
    pieces(0, 0, 3)
    ring_step(0, 0)
    mid_scatter(0)
    pieces(0, 3, 8)
    ring_step(0, 1)
    base_gu(1, 1)
    bt_out.wait_recv()
    bt_fwd.start()
    attend(1)
    ring_step(0, 2)
    gated(1)
    mid_gather(0)
    pieces(1, 0, 3)
    ring_step(1, 0)
    ring_step(0, 3)
    mid_scatter(1)
    pieces(1, 3, 8)
    ring_step(1, 1)
    bt_d2d.wait_recv()
    bt_fwd.wait_recv()
    lora_out(0)
    finish_y(0)
    ring_step(1, 2)
    mid_gather(1)
    ag_service(0, 0)
    ring_step(1, 3)
    ag_service(0, 1)
    lora_out(1)
    finish_y(1)
    ag_service(0, 2)
    ag_service(1, 0)
    ag_service(0, 3)
    ag_service(1, 1)
    ag_service(1, 2)
    ag_service(1, 3)
    for p in range(PASSES):
        for u in range(SUBS):
            for i in range(8):
                ag_d2d(p, i, u).wait_recv()

    for p in range(PASSES):
        for i in range(8):
            mid_d2d(p, i).wait_send()
            d2d(p, i).wait_send()
        for d in range(1, hch):
            mg_copy(p, d).wait_send()
        for d in range(1, chips):
            mid_send(p, d).wait_send()
        mid_part(p).wait_send()
        for way in range(2):
            for s in range(hch - way):
                mid_ring(p, way, s).wait_send()
                for u in range(SUBS):
                    ring_copy(p, way, s, u, 0).wait_send()
                    ag_ring(p, way, s, u).wait_send()
        for u in range(SUBS):
            for i in range(8):
                ag_d2d(p, i, u).wait_send()
    bt_out.wait_send()
    bt_d2d.wait_send()
    bt_fwd.wait_send()


def solution(mesh):
    n = mesh.shape['tensor']
    batch_spec = P('data', None, None)
    head_cols = P(None, 'tensor', None)
    head_rows = P('tensor', None, None)
    ff_cols = P(None, 'tensor')
    ff_rows = P('tensor', None)
    last_split = P(None, None, 'tensor')
    b_heads = P(None, None, 'tensor', None)
    a_heads = P(None, 'tensor', None, None)
    in_specs = (batch_spec, P('data'), P(None), head_cols, head_cols, head_cols, head_rows, ff_cols, ff_cols, ff_rows, last_split, b_heads, last_split, b_heads, last_split, b_heads, a_heads, last_split, last_split, last_split, last_split, last_split, head_cols, last_split)

    def local_layer(x_blk, adapter_ids, norm_gain, w_query, w_key, w_value, w_out, w_gate, w_up, w_down, a_query, b_query, a_key, b_key, a_value, b_value, a_out, b_out, a_gate, b_gate, a_up, b_up, a_down, b_down):
        seqs, seq, d_model = x_blk.shape
        tokens = seqs * seq
        n_adapt, _, rank = a_down.shape
        heads, head = w_query.shape[1:]
        wide = heads * head
        ff = w_gate.shape[1]
        chips = n // 2
        half = tokens // PASSES
        rows = half // 4
        cols = d_model // (chips // 2)
        mrows = 2 * rank // (chips // 2)
        share = rank // n

        hd = head // 2
        inv_freq = ROPE_BASE ** (-np.arange(hd, dtype=np.float32) / np.float32(hd))
        ang = inv_freq[:, None] * np.arange(seq, dtype=np.float32)[None, :]
        ang = np.tile(ang.astype(np.float32), (1, half // seq))
        cos_t, sin_t = jnp.asarray(np.cos(ang), F32), jnp.asarray(np.sin(ang), F32)

        def wt(w):
            return w.transpose(1, 2, 0).reshape(wide, d_model)

        def at(a):
            return a.transpose(0, 2, 1).reshape(n_adapt * share, d_model)

        def bt(b):
            return b.transpose(0, 2, 3, 1).reshape(n_adapt, wide, rank)

        args = (x_blk.reshape(tokens, d_model), adapter_ids, norm_gain.reshape(d_model // 128, 128), cos_t, sin_t,
                wt(w_query), wt(w_key), wt(w_value), w_out.reshape(wide, d_model), w_gate, w_up, w_down,
                at(a_query), at(a_key), at(a_value), at(a_gate), at(a_up),
                bt(b_query), bt(b_key), bt(b_value), b_gate.reshape(n_adapt * rank, ff), b_up.reshape(n_adapt * rank, ff),
                a_out.reshape(n_adapt, wide, rank), a_down, b_out.transpose(0, 2, 1), b_down.transpose(0, 2, 1))
        hbm = pl.BlockSpec(memory_space=pl.ANY)
        vmem = pl.BlockSpec(memory_space=pltpu.VMEM)
        dma = pltpu.SemaphoreType.DMA
        cfg = (n, tokens, seq, n_adapt, rank, heads, head, ff)
        scratch = [
            pltpu.SMEM((seqs,), jnp.int32),
            pltpu.VMEM((1, tokens), jnp.int32),
            pltpu.VMEM((d_model // 128, 128), F32),
            pltpu.VMEM((1, d_model), F32),
            pltpu.VMEM((hd, half), F32),
            pltpu.VMEM((hd, half), F32),
            pltpu.VMEM((tokens, d_model), BF16),
            pltpu.VMEM((tokens, d_model), BF16),
            pltpu.VMEM((5 * n_adapt * share, d_model), BF16),
            pltpu.VMEM((3 * wide, d_model), BF16),
            pltpu.VMEM((d_model, 2 * ff), BF16),
            pltpu.VMEM((3 * wide, n_adapt * rank), BF16),
            pltpu.VMEM((n_adapt * rank, 2 * ff), BF16),
            pltpu.VMEM((wide, d_model), BF16),
            pltpu.VMEM((ff, d_model), BF16),
            pltpu.VMEM((wide, n_adapt * rank), BF16),
            pltpu.VMEM((ff, n_adapt * rank), BF16),
            pltpu.VMEM((4 * wide, 2 * n_adapt * rank), BF16),
            pltpu.VMEM((3 * wide, tokens), F32),
            pltpu.VMEM((tokens, 2 * ff), F32),
            pltpu.VMEM((PASSES, n, 6 * share, half), BF16),
            pltpu.VMEM((n_adapt * rank, half), BF16),
            pltpu.VMEM((3 * wide, half), BF16),
            pltpu.VMEM((wide, tokens), BF16),
            pltpu.VMEM((tokens, ff), BF16),
            pltpu.VMEM((PASSES, 2, 2, 2 * rank, rows), BF16),
            pltpu.VMEM((PASSES, 2, 2 * rank, rows), BF16),
            pltpu.VMEM((PASSES, chips - 1, mrows, rows), BF16),
            pltpu.VMEM((PASSES, chips, 2, rows, cols), BF16),
            pltpu.VMEM((PASSES, chips, rows, cols), BF16),
            pltpu.VMEM((PASSES, 2, chips // 2, rows, cols), BF16),
            pltpu.VMEM((PASSES, chips // 2, mrows, rows), BF16),
            pltpu.VMEM((PASSES, rows, cols), F32),
            dma((56,)),
            dma((PASSES, 2, 4)), dma((PASSES, 2, 4)), dma((PASSES, 8)), dma((PASSES, 8)),
            dma((3,)), dma((3,)), dma((PASSES, 8)), dma((PASSES, 8)),
            dma((PASSES, 2, 4, SUBS)), dma((PASSES, 2, 4, SUBS)),
            dma((PASSES,)), dma((PASSES,)), dma((PASSES, chips - 1)), dma((PASSES, chips - 1)),
            dma((PASSES, 3)), dma((PASSES, 3)),
            dma((PASSES, 2, 4, SUBS)), dma((PASSES, 2, 4, SUBS)), dma((PASSES, 8, SUBS)), dma((PASSES, 8, SUBS)),
        ]
        y = pl.pallas_call(
            functools.partial(layer_kernel, cfg),
            out_shape=pltpu.VMEM((tokens, d_model), BF16),
            in_specs=[hbm] * 26,
            out_specs=vmem,
            scratch_shapes=scratch,
            compiler_params=pltpu.CompilerParams(collective_id=0, has_side_effects=True,
                                                 vmem_limit_bytes=59_000_000),
        )(*args)
        return y.reshape(x_blk.shape)

    return jax.shard_map(local_layer, mesh=mesh, in_specs=in_specs, out_specs=batch_spec, check_vma=False)
```

```python
import functools
import math

import jax
import jax.numpy as jnp
import numpy as np
from jax import lax
from jax.experimental import pallas as pl
from jax.experimental.pallas import tpu as pltpu
from jax.sharding import PartitionSpec as P

ALPHA = 16
EPS = 1e-5
ROPE_BASE = 10000.0
MESH = pl.DeviceIdType.MESH
F32 = jnp.float32
BF16 = jnp.bfloat16
PASSES = 2
SUBS = 2


def mm(lhs, rhs, lc=1, rc=0):
    return lax.dot_general(lhs, rhs, (((lc,), (rc,)), ((), ())), preferred_element_type=F32)


def layer_kernel(cfg, x_hbm, ids_hbm, gain_hbm, cos_hbm, sin_hbm,
                 wq, wk, wv, wo, wg, wu, wd,
                 aq, ak, av, ag, au, bq, bk, bv, bg, bu,
                 ao, ad, bo, bd, yv,
                 ids_s, ids_ref, gain_v, gain_ref, cos_ref, sin_ref, xv, hv, a_v, wqkv, wgu, bqkv, bgu, wo_v, wd_v, ao_v, ad_v, btg,
                 qkv_base, gu_base, gm, mmk, qk_v, ot_v, m_v, midp, midr, midx,
                 buf, drecv, ring, mg, xo,
                 ld, mf_s, mf_r, mid_s, mid_r, md_s, md_r, bt_s, bt_r, dd_s, dd_r, rg_s, rg_r,
                 mp_s, mp_r, mx_s, mx_r, mg_s, mg_r, ag_s, ag_r, ad_s, ad_r):
    n, tokens, seq, n_adapt, rank, heads, head, ff = cfg
    chips = n // 2
    half = tokens // PASSES
    wide = heads * head
    share = rank // n
    scale = ALPHA / rank
    d_model = xv.shape[1]
    cols = d_model // (chips // 2)
    rows = half // 4
    mrows = 2 * rank // (chips // 2)
    me = lax.axis_index('tensor')
    chip = me // 2
    core = lax.rem(me, 2)
    sign = 1 - 2 * core
    partner = 2 * chip + 1 - core

    def wrap(c):
        return lax.rem(c + 2 * chips, chips)

    def dev(c):
        return 2 * wrap(c) + core

    def rcopy(src, dst, ssem, rsem, to):
        return pltpu.make_async_remote_copy(src_ref=src, dst_ref=dst, send_sem=ssem, recv_sem=rsem,
                                            device_id={'tensor': to}, device_id_type=MESH)

    def drain_recv(ref, sem):
        rcopy(ref, ref, sem, sem, partner).wait_recv()

    def drain_send(ref, sem):
        rcopy(ref, ref, sem, sem, partner).wait_send()

    used = []

    def load(buffer, *pairs):
        sem = ld.at[len(used)]
        used.append(sem)
        for src, dst in pairs:
            pltpu.make_async_copy(src, dst, sem).start()
        return pltpu.make_async_copy(buffer, buffer, sem)

    tile = tokens // 4
    ids_ld = load(ids_s, (ids_hbm, ids_s))
    gain_ld = load(gain_v, (gain_hbm, gain_v))
    x_ld = [load(xv.at[pl.ds(i * tile, tile)], (x_hbm.at[pl.ds(i * tile, tile)], xv.at[pl.ds(i * tile, tile)])) for i in range(4)]
    a_rows = n_adapt * share
    a_ld = load(a_v, *((src, a_v.at[pl.ds(i * a_rows, a_rows)]) for i, src in enumerate((aq, ak, av, ag, au))))

    barrier = pltpu.get_barrier_semaphore()
    for step in range(1, n):
        pl.semaphore_signal(barrier, inc=1, device_id={'tensor': lax.rem(me + step, n)}, device_id_type=MESH)

    w1_ld = load(wqkv, *((src, wqkv.at[pl.ds(i * wide, wide)]) for i, src in enumerate((wq, wk, wv))))
    bt_rows = pl.ds(pl.multiple_of(lax.rem(me, 4) * wide, 16), wide)
    bt_ld = load(btg.at[bt_rows], *((src.at[a], btg.at[bt_rows, pl.ds((st * n_adapt + a) * rank, rank)])
                                    for st, src in enumerate((bo, bd)) for a in range(n_adapt)))
    w2_ld = load(wgu, *((src, wgu.at[:, pl.ds(i * ff, ff)]) for i, src in enumerate((wg, wu))))
    cos_ld = load(cos_ref, (cos_hbm, cos_ref))
    sin_ld = load(sin_ref, (sin_hbm, sin_ref))
    ids_ld.wait()
    gain_ld.wait()
    where_seq = lax.broadcasted_iota(jnp.int32, (1, tokens), 1) // seq
    ids_all = jnp.zeros((1, tokens), jnp.int32)
    for b in range(tokens // seq):
        ids_all = jnp.where(where_seq == b, ids_s[b], ids_all)
    ids_ref[...] = ids_all
    gain_ref[...] = jnp.concatenate([gain_v[b:b + 1, :] for b in range(gain_v.shape[0])], axis=1)

    nt = 128

    def norm_tiles(i):
        x_ld[i].wait()

        def body(j, carry):
            r = pl.ds(pl.multiple_of(i * tile + j * nt, nt), nt)
            xf = xv[r, :].astype(F32)
            inv = lax.rsqrt(jnp.mean(xf * xf, axis=-1, keepdims=True) + EPS)
            hv[r, :] = (xf * inv * gain_ref[...]).astype(BF16)
            return carry
        lax.fori_loop(0, tile // nt, body, 0)

    def mid_slot(hf, c, k):
        return gm.at[hf, 2 * wrap(c) + k]

    def mid_ring(hf, way, s):
        sg = sign if way == 0 else -sign
        slot = mid_slot(hf, chip - sg * s, core)
        return rcopy(slot, slot, mid_s.at[0], mid_r.at[way, s], dev(chip + sg))

    def mid_d2d(hf, i):
        if i == 0:
            c = chip
        elif i <= 4:
            c = chip - sign * i
        else:
            c = chip + sign * (i - 4)
        slot = mid_slot(hf, c, core)
        return rcopy(slot, slot, md_s.at[hf], md_r.at[hf], partner)

    def mid_direct(d):
        return rcopy(gm.at[0, me], gm.at[0, me], mf_s.at[0], mf_r.at[0], dev(chip + d))

    def mid_forward():
        drain_recv(gm.at[0, pl.ds(0, chips - 1)], mf_r.at[0])
        for i in range(1, 8):
            mid_d2d(0, i).start()

    hch = chips // 2

    def mid_service(hf, s):
        for way in range(2):
            last = hch - way
            if s < last:
                mid_ring(hf, way, s).wait_recv()
                if s + 1 < last:
                    mid_ring(hf, way, s + 1).start()
                mid_d2d(hf, (1 if way == 0 else 5) + s).start()

    def ids_of(start, size):
        return ids_ref[:, pl.ds(start, size)]

    def rank_part(hf):
        mids = mm(a_v[...], hv[pl.ds(hf * half, half), :], 1, 1)
        ids = ids_of(hf * half, half)
        out = []
        for st in range(5):
            acc = jnp.zeros((share, half), F32)
            for a in range(n_adapt):
                lo = (st * n_adapt + a) * share
                acc = jnp.where(ids == a, mids[lo:lo + share], acc)
            out += [acc[:, :half // 2], acc[:, half // 2:]]
        gm[hf, me] = jnp.concatenate(out, axis=0).astype(BF16)
        if hf == 0:
            pl.semaphore_wait(barrier, n - 1)
            for d in (4, 3, 5, 2, 6, 1, 7):
                mid_direct(d).start()
        else:
            mid_ring(hf, 0, 0).start()
            mid_ring(hf, 1, 0).start()
        mid_d2d(hf, 0).start()

    norm_tiles(0)
    norm_tiles(1)
    a_ld.wait()
    rank_part(0)
    norm_tiles(2)
    norm_tiles(3)
    rank_part(1)

    late = [
        load(bqkv, *((src.at[a], bqkv.at[pl.ds(i * wide, wide), pl.ds(a * rank, rank)])
                     for i, src in enumerate((bq, bk, bv)) for a in range(n_adapt))),
        load(bgu, *((src, bgu.at[:, pl.ds(i * ff, ff)]) for i, src in enumerate((bg, bu)))),
        load(wo_v, (wo, wo_v)),
        load(wd_v, (wd, wd_v)),
        load(ao_v, *((ao.at[a], ao_v.at[:, pl.ds(a * rank, rank)]) for a in range(n_adapt))),
        load(ad_v, *((ad.at[a], ad_v.at[:, pl.ds(a * rank, rank)]) for a in range(n_adapt))),
    ]
    def base_qkv(hf):
        r = pl.ds(hf * half, half)
        qkv_base[:, r] = mm(wqkv[...], hv[r, :], 1, 1)

    def base_gu(hf):
        r = pl.ds(hf * half, half)
        gu_base[r, :] = mm(hv[r, :], wgu[...])

    pair = chip + 1 - 2 * lax.rem(chip, 2)

    def bt_slot(dv):
        return btg.at[pl.ds(pl.multiple_of(lax.rem(dv, 4) * wide, 16), wide)]

    bt_half = n_adapt * rank

    def bt_out(st):
        slot = btg.at[pl.ds(pl.multiple_of(lax.rem(me, 4) * wide, 16), wide), pl.ds(st * bt_half, bt_half)]
        return rcopy(slot, slot, bt_s.at[0], bt_r.at[0], dev(pair))

    bt_d2d = rcopy(bt_slot(me), bt_slot(me), bt_s.at[0], bt_r.at[1], partner)
    bt_fwd = rcopy(bt_slot(dev(pair)), bt_slot(dev(pair)), bt_s.at[0], bt_r.at[2], partner)
    def build_mask(hf, st):
        ids = ids_of(hf * half, half)
        lo, hi = [], []
        for t in range(n):
            blk = gm[hf, t].astype(F32)
            lo.append(blk[2 * st * share:(2 * st + 1) * share])
            hi.append(blk[(2 * st + 1) * share:(2 * st + 2) * share])
        full = jnp.concatenate([jnp.concatenate(lo, axis=0), jnp.concatenate(hi, axis=0)], axis=1)
        for a in range(n_adapt):
            mmk[pl.ds(a * rank, rank), :] = jnp.where(ids == a, full, 0.0).astype(BF16)

    def attend(hf):
        drain_recv(gm.at[hf, pl.ds(0, chips)], md_r.at[hf])
        r = pl.ds(hf * half, half)
        hd = head // 2
        for st in range(3):
            build_mask(hf, st)
            w = pl.ds(st * wide, wide)
            z = qkv_base[w, r] + scale * mm(bqkv[w, :], mmk[...])
            if st < 2:
                out = []
                for h in range(heads):
                    first = z[h * head:h * head + hd]
                    second = z[h * head + hd:(h + 1) * head]
                    cs, sn = cos_ref[...], sin_ref[...]
                    out += [first * cs - second * sn, second * cs + first * sn]
                z = jnp.concatenate(out, axis=0)
            qk_v[w, :] = z.astype(BF16)
        blk = 256
        qi = lax.broadcasted_iota(jnp.int32, (blk, blk), 0)
        ki = lax.broadcasted_iota(jnp.int32, (blk, blk), 1)
        keep = (qi >= ki) & (qi // seq == ki // seq)
        for h in range(heads):
            for b in range(half // blk):
                c = pl.ds(b * blk, blk)
                qh = qk_v[pl.ds(h * head, head), c]
                kh = qk_v[pl.ds(wide + h * head, head), c]
                vh = qk_v[pl.ds(2 * wide + h * head, head), c]
                sc = mm(qh, kh, 0, 0) * (1.0 / math.sqrt(head))
                sc = jnp.where(keep, sc, -1e30)
                e = jnp.exp(sc - jnp.max(sc, axis=-1, keepdims=True))
                pr = (e * (1.0 / jnp.sum(e, axis=-1, keepdims=True))).astype(BF16)
                ot_v[pl.ds(h * head, head), pl.ds(hf * half + b * blk, blk)] = mm(vh, pr, 1, 1).astype(BF16)

    def pick(full, hf):
        ids = ids_of(hf * half, half)
        acc = jnp.zeros((rank, half), F32)
        for a in range(n_adapt):
            acc = jnp.where(ids == a, full[a * rank:(a + 1) * rank], acc)
        return acc.astype(BF16)

    def gated(hf):
        r = pl.ds(hf * half, half)
        for part in range(2):
            build_mask(hf, 3 + part)
            c = pl.ds(part * ff, ff)
            gu_base[r, c] = gu_base[r, c] + scale * mm(mmk[...], bgu[:, c], 0, 0)
        zg = gu_base[r, pl.ds(0, ff)]
        zu = gu_base[r, pl.ds(ff, ff)]
        m_v[r, :] = (zg / (1.0 + jnp.exp(-zg)) * zu).astype(BF16)
        for st, acc in enumerate((pick(mm(ao_v[...], ot_v[:, r], 0, 0), hf), pick(mm(ad_v[...], m_v[r, :], 0, 1), hf))):
            for q in range(4):
                midp[hf, q % 2, q // 2, pl.ds(st * rank, rank), :] = acc[:, q * rows:(q + 1) * rows]
        mid_part(hf).start()

    def mid_part(p):
        return rcopy(midp.at[p, 1 - core], midr.at[p], mp_s.at[p], mp_r.at[p], partner)

    def mid_block(p, c):
        c = wrap(c)
        return midp.at[p, core, lax.rem(c, 2), pl.ds(pl.multiple_of((c // 2) * mrows, mrows), mrows)]

    def mid_send(p, d):
        return rcopy(mid_block(p, chip + d), midx.at[p, d - 1], mx_s.at[p], mx_r.at[p], dev(chip + d))

    def mid_scatter(p):
        mid_part(p).wait_recv()
        midp[p, core] = (midp[p, core].astype(F32) + midr[p].astype(F32)).astype(BF16)
        for d in (4, 3, 5, 2, 6, 1, 7):
            mid_send(p, d).start()

    def mid_gather(p):
        tot = mid_block(p, chip)[...].astype(F32)
        drain_recv(midx.at[p], mx_r.at[p])
        for d in range(1, chips):
            tot = tot + midx[p, d - 1].astype(F32)
        mg[p, chip // 2] = tot.astype(BF16)
        for d in range(1, hch):
            mg_copy(p, d).start()

    def d2d(p, e):
        return rcopy(buf.at[p, e, 1 - core], drecv.at[p, e], dd_s.at[p], dd_r.at[p, e], partner)

    def group(p, g):
        c = pl.ds(pl.multiple_of(g * cols, 128), cols)
        r = pl.ds(p * half, half)
        val = mm(m_v[r, :], wd_v[:, c]) + mm(ot_v[:, r], wo_v[:, c], 0, 0)
        for q in range(4):
            buf[p, 2 * g + q // 2, q % 2] = val[q * rows:(q + 1) * rows].astype(BF16)
        d2d(p, 2 * g).start()
        d2d(p, 2 * g + 1).start()

    def groups(p, lo, hi):
        parity = lax.rem(chip, 2)
        own = chip // 2

        def body(t, carry):
            near = jnp.where(t == 1, 1 - 2 * parity, 2 * parity - 1)
            off = jnp.where(t == 0, 2, jnp.where(t == 3, 0, near))
            group(p, lax.rem(own + off + 4, 4))
            return carry
        lax.fori_loop(lo, hi, body, 0)

    def sub(u):
        return pl.ds(u * (rows // SUBS), rows // SUBS)

    def ring_dest(way, s):
        return wrap(chip + sign * (hch - s)) if way == 0 else wrap(chip - sign * (hch - 1 - s))

    def ring_copy(p, way, s, u):
        sg = sign if way == 0 else -sign
        return rcopy(buf.at[p, ring_dest(way, s), core, sub(u)], ring.at[p, way, s, sub(u)],
                     rg_s.at[p], rg_r.at[p, way, s, u], dev(chip + sg))

    met = set()

    def ring_part(p, way, s, u):
        e = ring_dest(way, s)
        if (p, way, s) not in met:
            met.add((p, way, s))
            d2d(p, e).wait_recv()
        tot = buf[p, e, core, sub(u)].astype(F32) + drecv[p, e, sub(u)].astype(F32)
        if s > 0:
            ring_copy(p, way, s - 1, u).wait_recv()
            tot = tot + ring[p, way, s - 1, sub(u)].astype(F32)
        buf[p, e, core, sub(u)] = tot.astype(BF16)
        ring_copy(p, way, s, u).start()

    def mg_copy(p, d):
        slot = mg.at[p, chip // 2]
        return rcopy(slot, slot, mg_s.at[p], mg_r.at[p], dev(chip + 2 * d))

    def y_rows(p, c, k, u):
        c = wrap(c)
        return pl.multiple_of(p * half + (2 * lax.rem(c, 2) + k) * rows + u * (rows // SUBS), rows // SUBS)

    def y_cols(c):
        return pl.ds(pl.multiple_of((wrap(c) // 2) * cols, 128), cols)

    def y_slot(p, c, k, u):
        return yv.at[pl.ds(y_rows(p, c, k, u), rows // SUBS), y_cols(c)]

    def ag_ring(p, way, s, u):
        sg = sign if way == 0 else -sign
        slot = y_slot(p, chip - sg * s, core, u)
        return rcopy(slot, slot, ag_s.at[p], ag_r.at[p, way, s, u], dev(chip + sg))

    def ag_d2d(p, i, u):
        if i == 0:
            c = chip
        elif i <= 4:
            c = chip - sign * i
        else:
            c = chip + sign * (i - 4)
        slot = y_slot(p, c, core, u)
        return rcopy(slot, slot, ad_s.at[p], ad_r.at[p], partner)

    def ag_part(p, way, s, u):
        ag_ring(p, way, s, u).wait_recv()
        if s + 1 < hch - way:
            ag_ring(p, way, s + 1, u).start()
        ag_d2d(p, (1 if way == 0 else 5) + s, u).start()

    def lora_out(p):
        drain_recv(midx.at[p, pl.ds(0, hch - 1)], mg_r.at[p])
        ids = ids_of(y_rows(p, chip, core, 0), rows)
        mids = jnp.concatenate([mg[p, g].astype(F32) for g in range(hch)], axis=0)
        parts = []
        for st in range(2):
            for a in range(n_adapt):
                parts.append(jnp.where(ids == a, mids[st * rank:(st + 1) * rank], 0.0).astype(BF16))
        lora = mm(jnp.concatenate(parts, axis=0), btg[...], 0, 1)
        r = pl.ds(y_rows(p, chip, core, 0), rows)
        xo[p] = xv[r, y_cols(chip)].astype(F32) + scale * lora

    def finish_part(p, u):
        if (p, 2, 0) not in met:
            met.add((p, 2, 0))
            d2d(p, chip).wait_recv()
        tot = buf[p, chip, core, sub(u)].astype(F32) + drecv[p, chip, sub(u)].astype(F32)
        for way in range(2):
            ring_copy(p, way, hch - 1 - way, u).wait_recv()
            tot = tot + ring[p, way, hch - 1 - way, sub(u)].astype(F32)
        y_slot(p, chip, core, u)[...] = (xo[p, sub(u)] + tot).astype(BF16)
        ag_ring(p, 0, 0, u).start()
        ag_ring(p, 1, 0, u).start()
        ag_d2d(p, 0, u).start()

    def bt_forward():
        drain_recv(btg.at[pl.ds(0, wide)], bt_r.at[0])
        bt_fwd.start()

    def bt_arrived():
        bt_d2d.wait_recv()
        bt_fwd.wait_recv()

    def rank_sends_done():
        drain_send(gm.at[0, pl.ds(0, chips - 1)], mf_s.at[0])
        drain_send(gm.at[0, pl.ds(0, chips - 1)], mid_s.at[0])
        for p in range(PASSES):
            drain_send(gm.at[p, pl.ds(0, chips)], md_s.at[p])
        drain_send(btg.at[pl.ds(0, 3 * wide)], bt_s.at[0])

    def sum_sends_done(p):
        drain_send(drecv.at[p], dd_s.at[p])
        drain_send(midx.at[p, pl.ds(0, hch - 1)], mg_s.at[p])
        drain_send(midx.at[p], mx_s.at[p])
        mid_part(p).wait_send()
        drain_send(drecv.at[p, pl.ds(0, chips - 1)], rg_s.at[p])

    def y_sends_done(p):
        drain_send(drecv.at[p, pl.ds(0, chips - 1)], ag_s.at[p])
        drain_send(drecv.at[p], ad_s.at[p])

    def y_arrived(p):
        drain_recv(drecv.at[p], ad_r.at[p])

    w1_ld.wait()
    base_qkv(0)
    bt_ld.wait()
    bt_out(0).start()
    bt_d2d.start()
    w2_ld.wait()
    base_gu(0)
    bt_out(1).start()
    base_qkv(1)
    mid_forward()
    mid_service(1, 0)
    for cp in [cos_ld, sin_ld] + late:
        cp.wait()
    attend(0)
    gated(0)
    groups(0, 0, 2)
    mid_service(1, 1)
    mid_scatter(0)
    bt_forward()
    groups(0, 2, 4)
    ring_part(0, 0, 0, 0)
    ring_part(0, 1, 0, 0)
    ring_part(0, 0, 0, 1)
    ring_part(0, 1, 0, 1)
    base_gu(1)
    mid_service(1, 2)
    ring_part(0, 1, 1, 0)
    ring_part(0, 0, 1, 0)
    ring_part(0, 1, 1, 1)
    mid_gather(0)
    ring_part(0, 0, 1, 1)
    mid_service(1, 3)
    attend(1)
    ring_part(0, 0, 2, 0)
    ring_part(0, 1, 2, 0)
    gated(1)
    mid_scatter(1)
    groups(1, 0, 2)
    bt_arrived()
    lora_out(0)
    ring_part(0, 0, 2, 1)
    ring_part(0, 1, 2, 1)
    ring_part(0, 0, 3, 0)
    groups(1, 2, 4)
    ring_part(1, 0, 0, 1)
    ring_part(1, 0, 0, 0)
    ring_part(1, 1, 0, 0)
    ring_part(1, 1, 0, 1)
    ring_part(0, 0, 3, 1)
    mid_gather(1)
    finish_part(0, 0)
    ring_part(1, 1, 1, 0)
    ring_part(1, 0, 1, 1)
    ring_part(1, 1, 1, 1)
    ring_part(1, 0, 1, 0)
    finish_part(0, 1)
    ag_part(0, 1, 0, 0)
    ring_part(1, 1, 2, 0)
    ag_part(0, 0, 0, 0)
    lora_out(1)
    ring_part(1, 1, 2, 1)
    ring_part(1, 0, 2, 1)
    ag_part(0, 1, 0, 1)
    ring_part(1, 0, 2, 0)
    ag_part(0, 1, 1, 0)
    ag_part(0, 0, 0, 1)
    ag_part(0, 0, 1, 0)
    ring_part(1, 0, 3, 1)
    ag_part(0, 1, 1, 1)
    ring_part(1, 0, 3, 0)
    ag_part(0, 1, 2, 0)
    ag_part(0, 0, 1, 1)
    ag_part(0, 0, 2, 0)
    ag_part(0, 1, 2, 1)
    finish_part(1, 1)
    finish_part(1, 0)
    ag_part(0, 0, 2, 1)
    ag_part(0, 0, 3, 0)
    ag_part(1, 1, 0, 1)
    ag_part(1, 0, 0, 1)
    ag_part(1, 1, 0, 0)
    ag_part(1, 0, 0, 0)
    ag_part(0, 0, 3, 1)
    ag_part(1, 1, 1, 1)
    ag_part(1, 0, 1, 1)
    ag_part(1, 1, 1, 0)
    ag_part(1, 0, 1, 0)
    ag_part(1, 1, 2, 1)
    ag_part(1, 0, 2, 1)
    ag_part(1, 1, 2, 0)
    ag_part(1, 0, 2, 0)
    ag_part(1, 0, 3, 1)
    ag_part(1, 0, 3, 0)
    rank_sends_done()
    for p in range(PASSES):
        sum_sends_done(p)
        y_arrived(p)
        y_sends_done(p)


def solution(mesh):
    n = mesh.shape['tensor']
    batch_spec = P('data', None, None)
    head_cols = P(None, 'tensor', None)
    head_rows = P('tensor', None, None)
    ff_cols = P(None, 'tensor')
    ff_rows = P('tensor', None)
    last_split = P(None, None, 'tensor')
    b_heads = P(None, None, 'tensor', None)
    a_heads = P(None, 'tensor', None, None)
    in_specs = (batch_spec, P('data'), P(None), head_cols, head_cols, head_cols, head_rows, ff_cols, ff_cols, ff_rows, last_split, b_heads, last_split, b_heads, last_split, b_heads, a_heads, last_split, last_split, last_split, last_split, last_split, head_cols, last_split)

    def local_layer(x_blk, adapter_ids, norm_gain, w_query, w_key, w_value, w_out, w_gate, w_up, w_down, a_query, b_query, a_key, b_key, a_value, b_value, a_out, b_out, a_gate, b_gate, a_up, b_up, a_down, b_down):
        seqs, seq, d_model = x_blk.shape
        tokens = seqs * seq
        n_adapt, _, rank = a_down.shape
        heads, head = w_query.shape[1:]
        wide = heads * head
        ff = w_gate.shape[1]
        chips = n // 2
        half = tokens // PASSES
        rows = half // 4
        cols = d_model // (chips // 2)
        mrows = 2 * rank // (chips // 2)
        share = rank // n

        hd = head // 2
        inv_freq = ROPE_BASE ** (-np.arange(hd, dtype=np.float32) / np.float32(hd))
        ang = inv_freq[:, None] * np.arange(seq, dtype=np.float32)[None, :]
        ang = np.tile(ang.astype(np.float32), (1, half // seq))
        cos_t, sin_t = jnp.asarray(np.cos(ang), F32), jnp.asarray(np.sin(ang), F32)

        def wt(w):
            return w.transpose(1, 2, 0).reshape(wide, d_model)

        def at(a):
            return a.transpose(0, 2, 1).reshape(n_adapt * share, d_model)

        def bt(b):
            return b.transpose(0, 2, 3, 1).reshape(n_adapt, wide, rank)

        args = (x_blk.reshape(tokens, d_model), adapter_ids, norm_gain.reshape(d_model // 128, 128), cos_t, sin_t,
                wt(w_query), wt(w_key), wt(w_value), w_out.reshape(wide, d_model), w_gate, w_up, w_down,
                at(a_query), at(a_key), at(a_value), at(a_gate), at(a_up),
                bt(b_query), bt(b_key), bt(b_value), b_gate.reshape(n_adapt * rank, ff), b_up.reshape(n_adapt * rank, ff),
                a_out.reshape(n_adapt, wide, rank), a_down, b_out.transpose(0, 2, 1), b_down.transpose(0, 2, 1))
        hbm = pl.BlockSpec(memory_space=pl.ANY)
        vmem = pl.BlockSpec(memory_space=pltpu.VMEM)
        dma = pltpu.SemaphoreType.DMA
        cfg = (n, tokens, seq, n_adapt, rank, heads, head, ff)
        scratch = [
            pltpu.SMEM((seqs,), jnp.int32),
            pltpu.VMEM((1, tokens), jnp.int32),
            pltpu.VMEM((d_model // 128, 128), F32),
            pltpu.VMEM((1, d_model), F32),
            pltpu.VMEM((hd, half), F32),
            pltpu.VMEM((hd, half), F32),
            pltpu.VMEM((tokens, d_model), BF16),
            pltpu.VMEM((tokens, d_model), BF16),
            pltpu.VMEM((5 * n_adapt * share, d_model), BF16),
            pltpu.VMEM((3 * wide, d_model), BF16),
            pltpu.VMEM((d_model, 2 * ff), BF16),
            pltpu.VMEM((3 * wide, n_adapt * rank), BF16),
            pltpu.VMEM((n_adapt * rank, 2 * ff), BF16),
            pltpu.VMEM((wide, d_model), BF16),
            pltpu.VMEM((ff, d_model), BF16),
            pltpu.VMEM((wide, n_adapt * rank), BF16),
            pltpu.VMEM((ff, n_adapt * rank), BF16),
            pltpu.VMEM((4 * wide, 2 * n_adapt * rank), BF16),
            pltpu.VMEM((3 * wide, tokens), F32),
            pltpu.VMEM((tokens, 2 * ff), F32),
            pltpu.VMEM((PASSES, n, 10 * share, half // 2), BF16),
            pltpu.VMEM((n_adapt * rank, half), BF16),
            pltpu.VMEM((3 * wide, half), BF16),
            pltpu.VMEM((wide, tokens), BF16),
            pltpu.VMEM((tokens, ff), BF16),
            pltpu.VMEM((PASSES, 2, 2, 2 * rank, rows), BF16),
            pltpu.VMEM((PASSES, 2, 2 * rank, rows), BF16),
            pltpu.VMEM((PASSES, chips - 1, mrows, rows), BF16),
            pltpu.VMEM((PASSES, chips, 2, rows, cols), BF16),
            pltpu.VMEM((PASSES, chips, rows, cols), BF16),
            pltpu.VMEM((PASSES, 2, chips // 2, rows, cols), BF16),
            pltpu.VMEM((PASSES, chips // 2, mrows, rows), BF16),
            pltpu.VMEM((PASSES, rows, cols), F32),
            dma((18,)), dma((1,)), dma((1,)),
            dma((1,)), dma((2, 4)), dma((PASSES,)), dma((PASSES,)),
            dma((1,)), dma((3,)), dma((PASSES,)), dma((PASSES, chips)),
            dma((PASSES,)), dma((PASSES, 2, 4, SUBS)),
            dma((PASSES,)), dma((PASSES,)), dma((PASSES,)), dma((PASSES,)),
            dma((PASSES,)), dma((PASSES,)),
            dma((PASSES,)), dma((PASSES, 2, 4, SUBS)), dma((PASSES,)), dma((PASSES,)),
        ]
        y = pl.pallas_call(
            functools.partial(layer_kernel, cfg),
            out_shape=pltpu.VMEM((tokens, d_model), BF16),
            in_specs=[hbm] * 26,
            out_specs=vmem,
            scratch_shapes=scratch,
            compiler_params=pltpu.CompilerParams(collective_id=0, has_side_effects=True,
                                                 vmem_limit_bytes=59_000_000),
        )(*args)
        return y.reshape(x_blk.shape)

    return jax.shard_map(local_layer, mesh=mesh, in_specs=in_specs, out_specs=batch_spec, check_vma=False)
```

```python
import functools
import math

import jax
import jax.numpy as jnp
import numpy as np
from jax import lax
from jax.experimental import pallas as pl
from jax.experimental.pallas import tpu as pltpu
from jax.sharding import PartitionSpec as P

ALPHA = 16
EPS = 1e-5
ROPE_BASE = 10000.0
MESH = pl.DeviceIdType.MESH
F32 = jnp.float32
BF16 = jnp.bfloat16
PASSES = 2
SUBS = 2


def mm(lhs, rhs, lc=1, rc=0):
    return lax.dot_general(lhs, rhs, (((lc,), (rc,)), ((), ())), preferred_element_type=F32)


def layer_kernel(cfg, x_hbm, ids_hbm, gain_hbm, cos_hbm, sin_hbm,
                 wq, wk, wv, wo, wg, wu, wd,
                 aq, ak, av, ag, au, bq, bk, bv, bg, bu,
                 ao, ad, bo, bd, yv,
                 ids_s, ids_ref, gain_v, gain_ref, cos_ref, sin_ref, xv, hv, a_v, wqkv, wgu, bqkv, bgu, wo_v, wd_v, ao_v, ad_v, btg,
                 qkv_base, gu_base, gm, mmk, qk_v, ot_v, m_v, midp, midr, midx,
                 buf, drecv, ring, mg, xo,
                 ld, mf_s, mf_r, mid_s, mid_r, md_s, md_r, bt_s, bt_r, dd_s, dd_r, rg_s, rg_r,
                 mp_s, mp_r, mx_s, mx_r, mg_s, mg_r, ag_s, ag_r, ad_s, ad_r):
    n, tokens, seq, n_adapt, rank, heads, head, ff = cfg
    chips = n // 2
    half = tokens // PASSES
    wide = heads * head
    share = rank // n
    scale = ALPHA / rank
    d_model = xv.shape[1]
    cols = d_model // (chips // 2)
    rows = half // 4
    mrows = 2 * rank // (chips // 2)
    me = lax.axis_index('tensor')
    chip = me // 2
    core = lax.rem(me, 2)
    sign = 1 - 2 * core
    partner = 2 * chip + 1 - core

    def wrap(c):
        return lax.rem(c + 2 * chips, chips)

    def dev(c):
        return 2 * wrap(c) + core

    def rcopy(src, dst, ssem, rsem, to):
        return pltpu.make_async_remote_copy(src_ref=src, dst_ref=dst, send_sem=ssem, recv_sem=rsem,
                                            device_id={'tensor': to}, device_id_type=MESH)

    def drain_recv(ref, sem):
        rcopy(ref, ref, sem, sem, partner).wait_recv()

    def drain_send(ref, sem):
        rcopy(ref, ref, sem, sem, partner).wait_send()

    used = []

    def load(buffer, *pairs):
        sem = ld.at[len(used)]
        used.append(sem)
        for src, dst in pairs:
            pltpu.make_async_copy(src, dst, sem).start()
        return pltpu.make_async_copy(buffer, buffer, sem)

    tile = tokens // 4
    ids_ld = load(ids_s, (ids_hbm, ids_s))
    gain_ld = load(gain_v, (gain_hbm, gain_v))
    x_ld = [load(xv.at[pl.ds(i * tile, tile)], (x_hbm.at[pl.ds(i * tile, tile)], xv.at[pl.ds(i * tile, tile)])) for i in range(4)]
    a_rows = n_adapt * share
    a_ld = load(a_v, *((src, a_v.at[pl.ds(i * a_rows, a_rows)]) for i, src in enumerate((aq, ak, av, ag, au))))

    barrier = pltpu.get_barrier_semaphore()
    for step in range(1, n):
        pl.semaphore_signal(barrier, inc=1, device_id={'tensor': lax.rem(me + step, n)}, device_id_type=MESH)

    w1_ld = load(wqkv, *((src, wqkv.at[pl.ds(i * wide, wide)]) for i, src in enumerate((wq, wk, wv))))
    bt_rows = pl.ds(pl.multiple_of(lax.rem(me, 4) * wide, 16), wide)
    bt_ld = load(btg.at[bt_rows], *((src.at[a], btg.at[bt_rows, pl.ds((st * n_adapt + a) * rank, rank)])
                                    for st, src in enumerate((bo, bd)) for a in range(n_adapt)))
    w2_ld = load(wgu, *((src, wgu.at[:, pl.ds(i * ff, ff)]) for i, src in enumerate((wg, wu))))
    cos_ld = load(cos_ref, (cos_hbm, cos_ref))
    sin_ld = load(sin_ref, (sin_hbm, sin_ref))
    ids_ld.wait()
    gain_ld.wait()
    where_seq = lax.broadcasted_iota(jnp.int32, (1, tokens), 1) // seq
    ids_all = jnp.zeros((1, tokens), jnp.int32)
    for b in range(tokens // seq):
        ids_all = jnp.where(where_seq == b, ids_s[b], ids_all)
    ids_ref[...] = ids_all
    gain_ref[...] = jnp.concatenate([gain_v[b:b + 1, :] for b in range(gain_v.shape[0])], axis=1)

    nt = 128

    def norm_tiles(i):
        x_ld[i].wait()

        def body(j, carry):
            r = pl.ds(pl.multiple_of(i * tile + j * nt, nt), nt)
            xf = xv[r, :].astype(F32)
            inv = lax.rsqrt(jnp.mean(xf * xf, axis=-1, keepdims=True) + EPS)
            hv[r, :] = (xf * inv * gain_ref[...]).astype(BF16)
            return carry
        lax.fori_loop(0, tile // nt, body, 0)

    def mid_slot(hf, c, k):
        return gm.at[hf, 2 * wrap(c) + k]

    def mid_ring(hf, way, s):
        sg = sign if way == 0 else -sign
        slot = mid_slot(hf, chip - sg * s, core)
        return rcopy(slot, slot, mid_s.at[0], mid_r.at[way, s], dev(chip + sg))

    def mid_d2d(hf, i):
        if i == 0:
            c = chip
        elif i <= 4:
            c = chip - sign * i
        else:
            c = chip + sign * (i - 4)
        slot = mid_slot(hf, c, core)
        return rcopy(slot, slot, md_s.at[hf], md_r.at[hf], partner)

    def mid_direct(d):
        return rcopy(gm.at[0, me], gm.at[0, me], mf_s.at[0], mf_r.at[0], dev(chip + d))

    def mid_forward():
        drain_recv(gm.at[0, pl.ds(0, chips - 1)], mf_r.at[0])
        for i in range(1, 8):
            mid_d2d(0, i).start()

    hch = chips // 2

    def mid_service(hf, s):
        for way in range(2):
            last = hch - way
            if s < last:
                mid_ring(hf, way, s).wait_recv()
                if s + 1 < last:
                    mid_ring(hf, way, s + 1).start()
                mid_d2d(hf, (1 if way == 0 else 5) + s).start()

    def ids_of(start, size):
        return ids_ref[:, pl.ds(start, size)]

    def rank_part(hf):
        mids = mm(a_v[...], hv[pl.ds(hf * half, half), :], 1, 1)
        ids = ids_of(hf * half, half)
        out = []
        for st in range(5):
            acc = jnp.zeros((share, half), F32)
            for a in range(n_adapt):
                lo = (st * n_adapt + a) * share
                acc = jnp.where(ids == a, mids[lo:lo + share], acc)
            out += [acc[:, :half // 2], acc[:, half // 2:]]
        gm[hf, me] = jnp.concatenate(out, axis=0).astype(BF16)
        if hf == 0:
            pl.semaphore_wait(barrier, n - 1)
            for d in (4, 3, 5, 2, 6, 1, 7):
                mid_direct(d).start()
        else:
            mid_ring(hf, 0, 0).start()
            mid_ring(hf, 1, 0).start()
        mid_d2d(hf, 0).start()

    norm_tiles(0)
    norm_tiles(1)
    a_ld.wait()
    rank_part(0)
    norm_tiles(2)
    norm_tiles(3)
    rank_part(1)

    late = [
        load(bqkv, *((src.at[a], bqkv.at[pl.ds(i * wide, wide), pl.ds(a * rank, rank)])
                     for i, src in enumerate((bq, bk, bv)) for a in range(n_adapt))),
        load(bgu, *((src, bgu.at[:, pl.ds(i * ff, ff)]) for i, src in enumerate((bg, bu)))),
        load(wo_v, (wo, wo_v)),
        load(wd_v, (wd, wd_v)),
        load(ao_v, *((ao.at[a], ao_v.at[:, pl.ds(a * rank, rank)]) for a in range(n_adapt))),
        load(ad_v, *((ad.at[a], ad_v.at[:, pl.ds(a * rank, rank)]) for a in range(n_adapt))),
    ]
    def base_qkv(hf):
        r = pl.ds(hf * half, half)
        qkv_base[:, r] = mm(wqkv[...], hv[r, :], 1, 1)

    def base_gu(hf):
        r = pl.ds(hf * half, half)
        gu_base[r, :] = mm(hv[r, :], wgu[...])

    pair = chip + 1 - 2 * lax.rem(chip, 2)

    def bt_slot(dv):
        return btg.at[pl.ds(pl.multiple_of(lax.rem(dv, 4) * wide, 16), wide)]

    bt_half = n_adapt * rank

    def bt_out(st):
        slot = btg.at[pl.ds(pl.multiple_of(lax.rem(me, 4) * wide, 16), wide), pl.ds(st * bt_half, bt_half)]
        return rcopy(slot, slot, bt_s.at[0], bt_r.at[0], dev(pair))

    bt_d2d = rcopy(bt_slot(me), bt_slot(me), bt_s.at[0], bt_r.at[1], partner)
    bt_fwd = rcopy(bt_slot(dev(pair)), bt_slot(dev(pair)), bt_s.at[0], bt_r.at[2], partner)
    def build_mask(hf, st):
        ids = ids_of(hf * half, half)
        lo, hi = [], []
        for t in range(n):
            blk = gm[hf, t].astype(F32)
            lo.append(blk[2 * st * share:(2 * st + 1) * share])
            hi.append(blk[(2 * st + 1) * share:(2 * st + 2) * share])
        full = jnp.concatenate([jnp.concatenate(lo, axis=0), jnp.concatenate(hi, axis=0)], axis=1)
        for a in range(n_adapt):
            mmk[pl.ds(a * rank, rank), :] = jnp.where(ids == a, full, 0.0).astype(BF16)

    def attend(hf):
        drain_recv(gm.at[hf, pl.ds(0, chips)], md_r.at[hf])
        r = pl.ds(hf * half, half)
        hd = head // 2
        for st in range(3):
            build_mask(hf, st)
            w = pl.ds(st * wide, wide)
            z = qkv_base[w, r] + scale * mm(bqkv[w, :], mmk[...])
            if st < 2:
                out = []
                for h in range(heads):
                    first = z[h * head:h * head + hd]
                    second = z[h * head + hd:(h + 1) * head]
                    cs, sn = cos_ref[...], sin_ref[...]
                    out += [first * cs - second * sn, second * cs + first * sn]
                z = jnp.concatenate(out, axis=0)
            qk_v[w, :] = z.astype(BF16)
        blk = 256
        qi = lax.broadcasted_iota(jnp.int32, (blk, blk), 0)
        ki = lax.broadcasted_iota(jnp.int32, (blk, blk), 1)
        keep = (qi >= ki) & (qi // seq == ki // seq)
        for h in range(heads):
            for b in range(half // blk):
                c = pl.ds(b * blk, blk)
                qh = qk_v[pl.ds(h * head, head), c]
                kh = qk_v[pl.ds(wide + h * head, head), c]
                vh = qk_v[pl.ds(2 * wide + h * head, head), c]
                sc = mm(qh, kh, 0, 0) * (1.0 / math.sqrt(head))
                sc = jnp.where(keep, sc, -1e30)
                e = jnp.exp(sc - jnp.max(sc, axis=-1, keepdims=True))
                pr = (e * (1.0 / jnp.sum(e, axis=-1, keepdims=True))).astype(BF16)
                ot_v[pl.ds(h * head, head), pl.ds(hf * half + b * blk, blk)] = mm(vh, pr, 1, 1).astype(BF16)

    def pick(full, hf):
        ids = ids_of(hf * half, half)
        acc = jnp.zeros((rank, half), F32)
        for a in range(n_adapt):
            acc = jnp.where(ids == a, full[a * rank:(a + 1) * rank], acc)
        return acc.astype(BF16)

    def gated(hf):
        r = pl.ds(hf * half, half)
        for part in range(2):
            build_mask(hf, 3 + part)
            c = pl.ds(part * ff, ff)
            gu_base[r, c] = gu_base[r, c] + scale * mm(mmk[...], bgu[:, c], 0, 0)
        zg = gu_base[r, pl.ds(0, ff)]
        zu = gu_base[r, pl.ds(ff, ff)]
        m_v[r, :] = (zg / (1.0 + jnp.exp(-zg)) * zu).astype(BF16)
        for st, acc in enumerate((pick(mm(ao_v[...], ot_v[:, r], 0, 0), hf), pick(mm(ad_v[...], m_v[r, :], 0, 1), hf))):
            for q in range(4):
                midp[hf, q % 2, q // 2, pl.ds(st * rank, rank), :] = acc[:, q * rows:(q + 1) * rows]
        mid_part(hf).start()

    def mid_part(p):
        return rcopy(midp.at[p, 1 - core], midr.at[p], mp_s.at[p], mp_r.at[p], partner)

    def mid_block(p, c):
        c = wrap(c)
        return midp.at[p, core, lax.rem(c, 2), pl.ds(pl.multiple_of((c // 2) * mrows, mrows), mrows)]

    def mid_send(p, d):
        return rcopy(mid_block(p, chip + d), midx.at[p, d - 1], mx_s.at[p], mx_r.at[p], dev(chip + d))

    def mid_scatter(p):
        mid_part(p).wait_recv()
        midp[p, core] = (midp[p, core].astype(F32) + midr[p].astype(F32)).astype(BF16)
        for d in (4, 3, 5, 2, 6, 1, 7):
            mid_send(p, d).start()

    def mid_gather(p):
        tot = mid_block(p, chip)[...].astype(F32)
        drain_recv(midx.at[p], mx_r.at[p])
        for d in range(1, chips):
            tot = tot + midx[p, d - 1].astype(F32)
        mg[p, chip // 2] = tot.astype(BF16)
        for d in range(1, hch):
            mg_copy(p, d).start()

    def d2d(p, e):
        return rcopy(buf.at[p, e, 1 - core], drecv.at[p, e], dd_s.at[p], dd_r.at[p, e], partner)

    def group(p, g):
        c = pl.ds(pl.multiple_of(g * cols, 128), cols)
        r = pl.ds(p * half, half)
        val = mm(m_v[r, :], wd_v[:, c]) + mm(ot_v[:, r], wo_v[:, c], 0, 0)
        for q in range(4):
            buf[p, 2 * g + q // 2, q % 2] = val[q * rows:(q + 1) * rows].astype(BF16)
        d2d(p, 2 * g).start()
        d2d(p, 2 * g + 1).start()

    def groups(p, lo, hi):
        parity = lax.rem(chip, 2)
        own = chip // 2

        def body(t, carry):
            near = jnp.where(t == 1, 1 - 2 * parity, 2 * parity - 1)
            off = jnp.where(t == 0, 2, jnp.where(t == 3, 0, near))
            group(p, lax.rem(own + off + 4, 4))
            return carry
        lax.fori_loop(lo, hi, body, 0)

    def sub(u):
        return pl.ds(u * (rows // SUBS), rows // SUBS)

    def ring_dest(way, s):
        return wrap(chip + sign * (hch - s)) if way == 0 else wrap(chip - sign * (hch - 1 - s))

    def ring_copy(p, way, s, u):
        sg = sign if way == 0 else -sign
        return rcopy(buf.at[p, ring_dest(way, s), core, sub(u)], ring.at[p, way, s, sub(u)],
                     rg_s.at[p], rg_r.at[p, way, s, u], dev(chip + sg))

    met = set()

    def ring_part(p, way, s, u):
        e = ring_dest(way, s)
        if (p, way, s) not in met:
            met.add((p, way, s))
            d2d(p, e).wait_recv()
        tot = buf[p, e, core, sub(u)].astype(F32) + drecv[p, e, sub(u)].astype(F32)
        if s > 0:
            ring_copy(p, way, s - 1, u).wait_recv()
            tot = tot + ring[p, way, s - 1, sub(u)].astype(F32)
        buf[p, e, core, sub(u)] = tot.astype(BF16)
        ring_copy(p, way, s, u).start()

    def mg_copy(p, d):
        slot = mg.at[p, chip // 2]
        return rcopy(slot, slot, mg_s.at[p], mg_r.at[p], dev(chip + 2 * d))

    def y_rows(p, c, k, u):
        c = wrap(c)
        return pl.multiple_of(p * half + (2 * lax.rem(c, 2) + k) * rows + u * (rows // SUBS), rows // SUBS)

    def y_cols(c):
        return pl.ds(pl.multiple_of((wrap(c) // 2) * cols, 128), cols)

    def y_slot(p, c, k, u):
        return yv.at[pl.ds(y_rows(p, c, k, u), rows // SUBS), y_cols(c)]

    def ag_ring(p, way, s, u):
        sg = sign if way == 0 else -sign
        slot = y_slot(p, chip - sg * s, core, u)
        return rcopy(slot, slot, ag_s.at[p], ag_r.at[p, way, s, u], dev(chip + sg))

    def ag_d2d(p, i, u):
        if i == 0:
            c = chip
        elif i <= 4:
            c = chip - sign * i
        else:
            c = chip + sign * (i - 4)
        slot = y_slot(p, c, core, u)
        return rcopy(slot, slot, ad_s.at[p], ad_r.at[p], partner)

    def ag_part(p, way, s, u):
        ag_ring(p, way, s, u).wait_recv()
        if s + 1 < hch - way:
            ag_ring(p, way, s + 1, u).start()
        ag_d2d(p, (1 if way == 0 else 5) + s, u).start()

    def lora_out(p):
        drain_recv(midx.at[p, pl.ds(0, hch - 1)], mg_r.at[p])
        ids = ids_of(y_rows(p, chip, core, 0), rows)
        mids = jnp.concatenate([mg[p, g].astype(F32) for g in range(hch)], axis=0)
        parts = []
        for st in range(2):
            for a in range(n_adapt):
                parts.append(jnp.where(ids == a, mids[st * rank:(st + 1) * rank], 0.0).astype(BF16))
        lora = mm(jnp.concatenate(parts, axis=0), btg[...], 0, 1)
        r = pl.ds(y_rows(p, chip, core, 0), rows)
        xo[p] = xv[r, y_cols(chip)].astype(F32) + scale * lora

    def finish_part(p, u):
        if (p, 2, 0) not in met:
            met.add((p, 2, 0))
            d2d(p, chip).wait_recv()
        tot = buf[p, chip, core, sub(u)].astype(F32) + drecv[p, chip, sub(u)].astype(F32)
        for way in range(2):
            ring_copy(p, way, hch - 1 - way, u).wait_recv()
            tot = tot + ring[p, way, hch - 1 - way, sub(u)].astype(F32)
        y_slot(p, chip, core, u)[...] = (xo[p, sub(u)] + tot).astype(BF16)
        ag_ring(p, 0, 0, u).start()
        ag_ring(p, 1, 0, u).start()
        ag_d2d(p, 0, u).start()

    def bt_forward():
        drain_recv(btg.at[pl.ds(0, wide)], bt_r.at[0])
        bt_fwd.start()

    def bt_arrived():
        bt_d2d.wait_recv()
        bt_fwd.wait_recv()

    def rank_sends_done():
        drain_send(gm.at[0, pl.ds(0, chips - 1)], mf_s.at[0])
        drain_send(gm.at[0, pl.ds(0, chips - 1)], mid_s.at[0])
        for p in range(PASSES):
            drain_send(gm.at[p, pl.ds(0, chips)], md_s.at[p])
        drain_send(btg.at[pl.ds(0, 3 * wide)], bt_s.at[0])

    def sum_sends_done(p):
        drain_send(drecv.at[p], dd_s.at[p])
        drain_send(midx.at[p, pl.ds(0, hch - 1)], mg_s.at[p])
        drain_send(midx.at[p], mx_s.at[p])
        mid_part(p).wait_send()
        drain_send(drecv.at[p, pl.ds(0, chips - 1)], rg_s.at[p])

    def y_sends_done(p):
        drain_send(drecv.at[p, pl.ds(0, chips - 1)], ag_s.at[p])
        drain_send(drecv.at[p], ad_s.at[p])

    def y_arrived(p):
        drain_recv(drecv.at[p], ad_r.at[p])

    def ring_step(p, s):
        for u in range(SUBS):
            for way in range(2):
                if s < hch - way:
                    ring_part(p, way, s, u)

    def ag_step(p, s):
        for u in range(SUBS):
            for way in range(2):
                if s < hch - way:
                    ag_part(p, way, s, u)

    def finish_y(p):
        for u in range(SUBS):
            finish_part(p, u)

    w1_ld.wait()
    base_qkv(0)
    bt_ld.wait()
    bt_out(0).start()
    bt_d2d.start()
    w2_ld.wait()
    base_gu(0)
    base_qkv(1)
    mid_forward()
    mid_service(1, 0)
    bt_out(1).start()
    for cp in [cos_ld, sin_ld] + late:
        cp.wait()
    attend(0)
    gated(0)
    mid_service(1, 1)
    groups(0, 0, 2)
    groups(0, 2, 4)
    mid_service(1, 2)
    ring_step(0, 0)
    mid_scatter(0)
    base_gu(1)
    mid_service(1, 3)
    bt_forward()
    attend(1)
    ring_step(0, 1)
    gated(1)
    mid_gather(0)
    groups(1, 0, 2)
    ring_step(0, 2)
    groups(1, 2, 4)
    ring_step(1, 0)
    mid_scatter(1)
    bt_arrived()
    ring_step(1, 1)
    mid_gather(1)
    lora_out(0)
    ring_step(0, 3)
    ring_step(1, 2)
    finish_y(0)
    ring_step(1, 3)
    ag_step(0, 0)
    lora_out(1)
    finish_y(1)
    ag_step(0, 1)
    ag_step(1, 0)
    ag_step(0, 2)
    ag_step(1, 1)
    ag_step(0, 3)
    ag_step(1, 2)
    ag_step(1, 3)
    rank_sends_done()
    for p in range(PASSES):
        sum_sends_done(p)
        y_arrived(p)
        y_sends_done(p)


def solution(mesh):
    n = mesh.shape['tensor']
    batch_spec = P('data', None, None)
    head_cols = P(None, 'tensor', None)
    head_rows = P('tensor', None, None)
    ff_cols = P(None, 'tensor')
    ff_rows = P('tensor', None)
    last_split = P(None, None, 'tensor')
    b_heads = P(None, None, 'tensor', None)
    a_heads = P(None, 'tensor', None, None)
    in_specs = (batch_spec, P('data'), P(None), head_cols, head_cols, head_cols, head_rows, ff_cols, ff_cols, ff_rows, last_split, b_heads, last_split, b_heads, last_split, b_heads, a_heads, last_split, last_split, last_split, last_split, last_split, head_cols, last_split)

    def local_layer(x_blk, adapter_ids, norm_gain, w_query, w_key, w_value, w_out, w_gate, w_up, w_down, a_query, b_query, a_key, b_key, a_value, b_value, a_out, b_out, a_gate, b_gate, a_up, b_up, a_down, b_down):
        seqs, seq, d_model = x_blk.shape
        tokens = seqs * seq
        n_adapt, _, rank = a_down.shape
        heads, head = w_query.shape[1:]
        wide = heads * head
        ff = w_gate.shape[1]
        chips = n // 2
        half = tokens // PASSES
        rows = half // 4
        cols = d_model // (chips // 2)
        mrows = 2 * rank // (chips // 2)
        share = rank // n

        hd = head // 2
        inv_freq = ROPE_BASE ** (-np.arange(hd, dtype=np.float32) / np.float32(hd))
        ang = inv_freq[:, None] * np.arange(seq, dtype=np.float32)[None, :]
        ang = np.tile(ang.astype(np.float32), (1, half // seq))
        cos_t, sin_t = jnp.asarray(np.cos(ang), F32), jnp.asarray(np.sin(ang), F32)

        def wt(w):
            return w.transpose(1, 2, 0).reshape(wide, d_model)

        def at(a):
            return a.transpose(0, 2, 1).reshape(n_adapt * share, d_model)

        def bt(b):
            return b.transpose(0, 2, 3, 1).reshape(n_adapt, wide, rank)

        args = (x_blk.reshape(tokens, d_model), adapter_ids, norm_gain.reshape(d_model // 128, 128), cos_t, sin_t,
                wt(w_query), wt(w_key), wt(w_value), w_out.reshape(wide, d_model), w_gate, w_up, w_down,
                at(a_query), at(a_key), at(a_value), at(a_gate), at(a_up),
                bt(b_query), bt(b_key), bt(b_value), b_gate.reshape(n_adapt * rank, ff), b_up.reshape(n_adapt * rank, ff),
                a_out.reshape(n_adapt, wide, rank), a_down, b_out.transpose(0, 2, 1), b_down.transpose(0, 2, 1))
        hbm = pl.BlockSpec(memory_space=pl.ANY)
        vmem = pl.BlockSpec(memory_space=pltpu.VMEM)
        dma = pltpu.SemaphoreType.DMA
        cfg = (n, tokens, seq, n_adapt, rank, heads, head, ff)
        scratch = [
            pltpu.SMEM((seqs,), jnp.int32),
            pltpu.VMEM((1, tokens), jnp.int32),
            pltpu.VMEM((d_model // 128, 128), F32),
            pltpu.VMEM((1, d_model), F32),
            pltpu.VMEM((hd, half), F32),
            pltpu.VMEM((hd, half), F32),
            pltpu.VMEM((tokens, d_model), BF16),
            pltpu.VMEM((tokens, d_model), BF16),
            pltpu.VMEM((5 * n_adapt * share, d_model), BF16),
            pltpu.VMEM((3 * wide, d_model), BF16),
            pltpu.VMEM((d_model, 2 * ff), BF16),
            pltpu.VMEM((3 * wide, n_adapt * rank), BF16),
            pltpu.VMEM((n_adapt * rank, 2 * ff), BF16),
            pltpu.VMEM((wide, d_model), BF16),
            pltpu.VMEM((ff, d_model), BF16),
            pltpu.VMEM((wide, n_adapt * rank), BF16),
            pltpu.VMEM((ff, n_adapt * rank), BF16),
            pltpu.VMEM((4 * wide, 2 * n_adapt * rank), BF16),
            pltpu.VMEM((3 * wide, tokens), F32),
            pltpu.VMEM((tokens, 2 * ff), F32),
            pltpu.VMEM((PASSES, n, 10 * share, half // 2), BF16),
            pltpu.VMEM((n_adapt * rank, half), BF16),
            pltpu.VMEM((3 * wide, half), BF16),
            pltpu.VMEM((wide, tokens), BF16),
            pltpu.VMEM((tokens, ff), BF16),
            pltpu.VMEM((PASSES, 2, 2, 2 * rank, rows), BF16),
            pltpu.VMEM((PASSES, 2, 2 * rank, rows), BF16),
            pltpu.VMEM((PASSES, chips - 1, mrows, rows), BF16),
            pltpu.VMEM((PASSES, chips, 2, rows, cols), BF16),
            pltpu.VMEM((PASSES, chips, rows, cols), BF16),
            pltpu.VMEM((PASSES, 2, chips // 2, rows, cols), BF16),
            pltpu.VMEM((PASSES, chips // 2, mrows, rows), BF16),
            pltpu.VMEM((PASSES, rows, cols), F32),
            dma((18,)), dma((1,)), dma((1,)),
            dma((1,)), dma((2, 4)), dma((PASSES,)), dma((PASSES,)),
            dma((1,)), dma((3,)), dma((PASSES,)), dma((PASSES, chips)),
            dma((PASSES,)), dma((PASSES, 2, 4, SUBS)),
            dma((PASSES,)), dma((PASSES,)), dma((PASSES,)), dma((PASSES,)),
            dma((PASSES,)), dma((PASSES,)),
            dma((PASSES,)), dma((PASSES, 2, 4, SUBS)), dma((PASSES,)), dma((PASSES,)),
        ]
        y = pl.pallas_call(
            functools.partial(layer_kernel, cfg),
            out_shape=pltpu.VMEM((tokens, d_model), BF16),
            in_specs=[hbm] * 26,
            out_specs=vmem,
            scratch_shapes=scratch,
            compiler_params=pltpu.CompilerParams(collective_id=0, has_side_effects=True,
                                                 vmem_limit_bytes=59_000_000),
        )(*args)
        return y.reshape(x_blk.shape)

    return jax.shard_map(local_layer, mesh=mesh, in_specs=in_specs, out_specs=batch_spec, check_vma=False)
```

```python
import functools
import math

import jax
import jax.numpy as jnp
import numpy as np
from jax import lax
from jax.experimental import pallas as pl
from jax.experimental.pallas import tpu as pltpu
from jax.sharding import PartitionSpec as P

ALPHA = 16
EPS = 1e-5
ROPE_BASE = 10000.0
MESH = pl.DeviceIdType.MESH
F32 = jnp.float32
BF16 = jnp.bfloat16
PASSES = 2
SUBS = 2


def mm(lhs, rhs, lc=1, rc=0):
    return lax.dot_general(lhs, rhs, (((lc,), (rc,)), ((), ())), preferred_element_type=F32)


def layer_kernel(cfg, x_hbm, ids_hbm, gain_hbm, cos_hbm, sin_hbm,
                 wq, wk, wv, wo, wg, wu, wd,
                 aq, ak, av, ag, au, bq, bk, bv, bg, bu,
                 ao, ad, bo, bd, yv,
                 ids_s, ids_ref, gain_v, gain_ref, cos_ref, sin_ref, xv, hv, a_v, wqkv, wgu, bqkv, bgu, wo_v, wd_v, ao_v, ad_v, btg,
                 qkv_base, gu_base, gm, mmk, qk_v, ot_v, m_v, midp, midr, midx,
                 buf, drecv, ring, mg, xo,
                 ld, mf_s, mf_r, mid_s, mid_r, md_s, md_r, bt_s, bt_r, dd_s, dd_r, rg_s, rg_r,
                 mp_s, mp_r, mx_s, mx_r, mg_s, mg_r, ag_s, ag_r, ad_s, ad_r):
    n, tokens, seq, n_adapt, rank, heads, head, ff = cfg
    chips = n // 2
    half = tokens // PASSES
    wide = heads * head
    share = rank // n
    scale = ALPHA / rank
    d_model = xv.shape[1]
    cols = d_model // (chips // 2)
    rows = half // 4
    mrows = 2 * rank // (chips // 2)
    me = lax.axis_index('tensor')
    chip = me // 2
    core = lax.rem(me, 2)
    sign = 1 - 2 * core
    partner = 2 * chip + 1 - core

    def wrap(c):
        return lax.rem(c + 2 * chips, chips)

    def dev(c):
        return 2 * wrap(c) + core

    def rcopy(src, dst, ssem, rsem, to):
        return pltpu.make_async_remote_copy(src_ref=src, dst_ref=dst, send_sem=ssem, recv_sem=rsem,
                                            device_id={'tensor': to}, device_id_type=MESH)

    def drain_recv(ref, sem):
        rcopy(ref, ref, sem, sem, partner).wait_recv()

    def drain_send(ref, sem):
        rcopy(ref, ref, sem, sem, partner).wait_send()

    used = []

    def load(buffer, *pairs):
        sem = ld.at[len(used)]
        used.append(sem)
        for src, dst in pairs:
            pltpu.make_async_copy(src, dst, sem).start()
        return pltpu.make_async_copy(buffer, buffer, sem)

    tile = tokens // 4
    ids_ld = load(ids_s, (ids_hbm, ids_s))
    gain_ld = load(gain_v, (gain_hbm, gain_v))
    x_ld = [load(xv.at[pl.ds(i * tile, tile)], (x_hbm.at[pl.ds(i * tile, tile)], xv.at[pl.ds(i * tile, tile)])) for i in range(4)]
    a_rows = n_adapt * share
    a_ld = load(a_v, *((src, a_v.at[pl.ds(i * a_rows, a_rows)]) for i, src in enumerate((aq, ak, av, ag, au))))

    barrier = pltpu.get_barrier_semaphore()
    for step in range(1, n):
        pl.semaphore_signal(barrier, inc=1, device_id={'tensor': lax.rem(me + step, n)}, device_id_type=MESH)

    w1_ld = load(wqkv, *((src, wqkv.at[pl.ds(i * wide, wide)]) for i, src in enumerate((wq, wk, wv))))
    bt_rows = pl.ds(pl.multiple_of(lax.rem(me, 4) * wide, 16), wide)
    bt_ld = load(btg.at[bt_rows], *((src.at[a], btg.at[bt_rows, pl.ds((st * n_adapt + a) * rank, rank)])
                                    for st, src in enumerate((bo, bd)) for a in range(n_adapt)))
    w2_ld = load(wgu, *((src, wgu.at[:, pl.ds(i * ff, ff)]) for i, src in enumerate((wg, wu))))
    cos_ld = load(cos_ref, (cos_hbm, cos_ref))
    sin_ld = load(sin_ref, (sin_hbm, sin_ref))
    ids_ld.wait()
    gain_ld.wait()
    where_seq = lax.broadcasted_iota(jnp.int32, (1, tokens), 1) // seq
    ids_all = jnp.zeros((1, tokens), jnp.int32)
    for b in range(tokens // seq):
        ids_all = jnp.where(where_seq == b, ids_s[b], ids_all)
    ids_ref[...] = ids_all
    gain_ref[...] = jnp.concatenate([gain_v[b:b + 1, :] for b in range(gain_v.shape[0])], axis=1)

    nt = 128

    def norm_tiles(i):
        x_ld[i].wait()

        def body(j, carry):
            r = pl.ds(pl.multiple_of(i * tile + j * nt, nt), nt)
            xf = xv[r, :].astype(F32)
            inv = lax.rsqrt(jnp.mean(xf * xf, axis=-1, keepdims=True) + EPS)
            hv[r, :] = (xf * inv * gain_ref[...]).astype(BF16)
            return carry
        lax.fori_loop(0, tile // nt, body, 0)

    def mid_slot(hf, c, k):
        return gm.at[hf, 2 * wrap(c) + k]

    def mid_ring(hf, way, s):
        sg = sign if way == 0 else -sign
        slot = mid_slot(hf, chip - sg * s, core)
        return rcopy(slot, slot, mid_s.at[0], mid_r.at[way, s], dev(chip + sg))

    def mid_d2d(hf, i):
        if i == 0:
            c = chip
        elif i <= 4:
            c = chip - sign * i
        else:
            c = chip + sign * (i - 4)
        slot = mid_slot(hf, c, core)
        return rcopy(slot, slot, md_s.at[hf], md_r.at[hf], partner)

    def mid_direct(d):
        return rcopy(gm.at[0, me], gm.at[0, me], mf_s.at[0], mf_r.at[0], dev(chip + d))

    def mid_forward():
        drain_recv(gm.at[0, pl.ds(0, chips - 1)], mf_r.at[0])
        for i in range(1, 8):
            mid_d2d(0, i).start()

    hch = chips // 2

    def mid_service(hf, s):
        for way in range(2):
            last = hch - way
            if s < last:
                mid_ring(hf, way, s).wait_recv()
                if s + 1 < last:
                    mid_ring(hf, way, s + 1).start()
                mid_d2d(hf, (1 if way == 0 else 5) + s).start()

    def ids_of(start, size):
        return ids_ref[:, pl.ds(start, size)]

    def rank_part(hf):
        mids = mm(a_v[...], hv[pl.ds(hf * half, half), :], 1, 1)
        ids = ids_of(hf * half, half)
        out = []
        for st in range(5):
            acc = jnp.zeros((share, half), F32)
            for a in range(n_adapt):
                lo = (st * n_adapt + a) * share
                acc = jnp.where(ids == a, mids[lo:lo + share], acc)
            out += [acc[:, :half // 2], acc[:, half // 2:]]
        gm[hf, me] = jnp.concatenate(out, axis=0).astype(BF16)
        if hf == 0:
            pl.semaphore_wait(barrier, n - 1)
            for d in (4, 3, 5, 2, 6, 1, 7):
                mid_direct(d).start()
        else:
            mid_ring(hf, 0, 0).start()
            mid_ring(hf, 1, 0).start()
        mid_d2d(hf, 0).start()

    norm_tiles(0)
    norm_tiles(1)
    a_ld.wait()
    rank_part(0)
    norm_tiles(2)
    norm_tiles(3)
    rank_part(1)

    late = [
        load(bqkv, *((src.at[a], bqkv.at[pl.ds(i * wide, wide), pl.ds(a * rank, rank)])
                     for i, src in enumerate((bq, bk, bv)) for a in range(n_adapt))),
        load(bgu, *((src, bgu.at[:, pl.ds(i * ff, ff)]) for i, src in enumerate((bg, bu)))),
        load(wo_v, (wo, wo_v)),
        load(wd_v, (wd, wd_v)),
        load(ao_v, *((ao.at[a], ao_v.at[:, pl.ds(a * rank, rank)]) for a in range(n_adapt))),
        load(ad_v, *((ad.at[a], ad_v.at[:, pl.ds(a * rank, rank)]) for a in range(n_adapt))),
    ]
    def base_qkv(hf):
        r = pl.ds(hf * half, half)
        qkv_base[:, r] = mm(wqkv[...], hv[r, :], 1, 1)

    def base_gu(hf):
        r = pl.ds(hf * half, half)
        gu_base[r, :] = mm(hv[r, :], wgu[...])

    pair = chip + 1 - 2 * lax.rem(chip, 2)

    def bt_slot(dv):
        return btg.at[pl.ds(pl.multiple_of(lax.rem(dv, 4) * wide, 16), wide)]

    bt_half = n_adapt * rank

    def bt_out(st):
        slot = btg.at[pl.ds(pl.multiple_of(lax.rem(me, 4) * wide, 16), wide), pl.ds(st * bt_half, bt_half)]
        return rcopy(slot, slot, bt_s.at[0], bt_r.at[0], dev(pair))

    bt_d2d = rcopy(bt_slot(me), bt_slot(me), bt_s.at[0], bt_r.at[1], partner)
    bt_fwd = rcopy(bt_slot(dev(pair)), bt_slot(dev(pair)), bt_s.at[0], bt_r.at[2], partner)
    def build_mask(hf, st):
        ids = ids_of(hf * half, half)
        lo, hi = [], []
        for t in range(n):
            blk = gm[hf, t].astype(F32)
            lo.append(blk[2 * st * share:(2 * st + 1) * share])
            hi.append(blk[(2 * st + 1) * share:(2 * st + 2) * share])
        full = jnp.concatenate([jnp.concatenate(lo, axis=0), jnp.concatenate(hi, axis=0)], axis=1)
        for a in range(n_adapt):
            mmk[pl.ds(a * rank, rank), :] = jnp.where(ids == a, full, 0.0).astype(BF16)

    def attend(hf):
        drain_recv(gm.at[hf, pl.ds(0, chips)], md_r.at[hf])
        r = pl.ds(hf * half, half)
        hd = head // 2
        for st in range(3):
            build_mask(hf, st)
            w = pl.ds(st * wide, wide)
            z = qkv_base[w, r] + scale * mm(bqkv[w, :], mmk[...])
            if st < 2:
                out = []
                for h in range(heads):
                    first = z[h * head:h * head + hd]
                    second = z[h * head + hd:(h + 1) * head]
                    cs, sn = cos_ref[...], sin_ref[...]
                    out += [first * cs - second * sn, second * cs + first * sn]
                z = jnp.concatenate(out, axis=0)
            qk_v[w, :] = z.astype(BF16)
        blk = 256
        qi = lax.broadcasted_iota(jnp.int32, (blk, blk), 0)
        ki = lax.broadcasted_iota(jnp.int32, (blk, blk), 1)
        keep = (qi >= ki) & (qi // seq == ki // seq)
        for h in range(heads):
            for b in range(half // blk):
                c = pl.ds(b * blk, blk)
                qh = qk_v[pl.ds(h * head, head), c]
                kh = qk_v[pl.ds(wide + h * head, head), c]
                vh = qk_v[pl.ds(2 * wide + h * head, head), c]
                sc = mm(qh, kh, 0, 0) * (1.0 / math.sqrt(head))
                sc = jnp.where(keep, sc, -1e30)
                e = jnp.exp(sc - jnp.max(sc, axis=-1, keepdims=True))
                pr = (e * (1.0 / jnp.sum(e, axis=-1, keepdims=True))).astype(BF16)
                ot_v[pl.ds(h * head, head), pl.ds(hf * half + b * blk, blk)] = mm(vh, pr, 1, 1).astype(BF16)

    def pick(full, hf):
        ids = ids_of(hf * half, half)
        acc = jnp.zeros((rank, half), F32)
        for a in range(n_adapt):
            acc = jnp.where(ids == a, full[a * rank:(a + 1) * rank], acc)
        return acc.astype(BF16)

    def gated(hf):
        r = pl.ds(hf * half, half)
        for part in range(2):
            build_mask(hf, 3 + part)
            c = pl.ds(part * ff, ff)
            gu_base[r, c] = gu_base[r, c] + scale * mm(mmk[...], bgu[:, c], 0, 0)
        zg = gu_base[r, pl.ds(0, ff)]
        zu = gu_base[r, pl.ds(ff, ff)]
        m_v[r, :] = (zg / (1.0 + jnp.exp(-zg)) * zu).astype(BF16)
        for st, acc in enumerate((pick(mm(ao_v[...], ot_v[:, r], 0, 0), hf), pick(mm(ad_v[...], m_v[r, :], 0, 1), hf))):
            for q in range(4):
                midp[hf, q % 2, q // 2, pl.ds(st * rank, rank), :] = acc[:, q * rows:(q + 1) * rows]
        mid_part(hf).start()

    def mid_part(p):
        return rcopy(midp.at[p, 1 - core], midr.at[p], mp_s.at[p], mp_r.at[p], partner)

    def mid_block(p, c):
        c = wrap(c)
        return midp.at[p, core, lax.rem(c, 2), pl.ds(pl.multiple_of((c // 2) * mrows, mrows), mrows)]

    def mid_send(p, d):
        return rcopy(mid_block(p, chip + d), midx.at[p, d - 1], mx_s.at[p], mx_r.at[p], dev(chip + d))

    def mid_scatter(p):
        mid_part(p).wait_recv()
        midp[p, core] = (midp[p, core].astype(F32) + midr[p].astype(F32)).astype(BF16)
        for d in (4, 3, 5, 2, 6, 1, 7):
            mid_send(p, d).start()

    def mid_gather(p):
        tot = mid_block(p, chip)[...].astype(F32)
        drain_recv(midx.at[p], mx_r.at[p])
        for d in range(1, chips):
            tot = tot + midx[p, d - 1].astype(F32)
        mg[p, chip // 2] = tot.astype(BF16)
        for d in range(1, hch):
            mg_copy(p, d).start()

    def d2d(p, e):
        return rcopy(buf.at[p, e, 1 - core], drecv.at[p, e], dd_s.at[p], dd_r.at[p, e], partner)

    def group(p, g):
        c = pl.ds(pl.multiple_of(g * cols, 128), cols)
        r = pl.ds(p * half, half)
        val = mm(m_v[r, :], wd_v[:, c]) + mm(ot_v[:, r], wo_v[:, c], 0, 0)
        for q in range(4):
            buf[p, 2 * g + q // 2, q % 2] = val[q * rows:(q + 1) * rows].astype(BF16)
        d2d(p, 2 * g).start()
        d2d(p, 2 * g + 1).start()

    def groups(p, lo, hi):
        parity = lax.rem(chip, 2)
        own = chip // 2

        def body(t, carry):
            near = jnp.where(t == 1, 1 - 2 * parity, 2 * parity - 1)
            off = jnp.where(t == 0, 2, jnp.where(t == 3, 0, near))
            group(p, lax.rem(own + off + 4, 4))
            return carry
        lax.fori_loop(lo, hi, body, 0)

    def sub(u):
        return pl.ds(u * (rows // SUBS), rows // SUBS)

    def ring_dest(way, s):
        return wrap(chip + sign * (hch - s)) if way == 0 else wrap(chip - sign * (hch - 1 - s))

    def ring_copy(p, way, s, u):
        sg = sign if way == 0 else -sign
        return rcopy(buf.at[p, ring_dest(way, s), core, sub(u)], ring.at[p, way, s, sub(u)],
                     rg_s.at[p], rg_r.at[p, way, s, u], dev(chip + sg))

    met = set()

    def ring_part(p, way, s, u):
        e = ring_dest(way, s)
        if (p, way, s) not in met:
            met.add((p, way, s))
            d2d(p, e).wait_recv()
        tot = buf[p, e, core, sub(u)].astype(F32) + drecv[p, e, sub(u)].astype(F32)
        if s > 0:
            ring_copy(p, way, s - 1, u).wait_recv()
            tot = tot + ring[p, way, s - 1, sub(u)].astype(F32)
        buf[p, e, core, sub(u)] = tot.astype(BF16)
        ring_copy(p, way, s, u).start()

    def mg_copy(p, d):
        slot = mg.at[p, chip // 2]
        return rcopy(slot, slot, mg_s.at[p], mg_r.at[p], dev(chip + 2 * d))

    def y_rows(p, c, k, u):
        c = wrap(c)
        return pl.multiple_of(p * half + (2 * lax.rem(c, 2) + k) * rows + u * (rows // SUBS), rows // SUBS)

    def y_cols(c):
        return pl.ds(pl.multiple_of((wrap(c) // 2) * cols, 128), cols)

    def y_slot(p, c, k, u):
        return yv.at[pl.ds(y_rows(p, c, k, u), rows // SUBS), y_cols(c)]

    def ag_ring(p, way, s, u):
        sg = sign if way == 0 else -sign
        slot = y_slot(p, chip - sg * s, core, u)
        return rcopy(slot, slot, ag_s.at[p], ag_r.at[p, way, s, u], dev(chip + sg))

    def ag_d2d(p, i, u):
        if i == 0:
            c = chip
        elif i <= 4:
            c = chip - sign * i
        else:
            c = chip + sign * (i - 4)
        slot = y_slot(p, c, core, u)
        return rcopy(slot, slot, ad_s.at[p], ad_r.at[p], partner)

    def ag_part(p, way, s, u):
        ag_ring(p, way, s, u).wait_recv()
        if s + 1 < hch - way:
            ag_ring(p, way, s + 1, u).start()
        ag_d2d(p, (1 if way == 0 else 5) + s, u).start()

    def lora_out(p):
        drain_recv(midx.at[p, pl.ds(0, hch - 1)], mg_r.at[p])
        ids = ids_of(y_rows(p, chip, core, 0), rows)
        mids = jnp.concatenate([mg[p, g].astype(F32) for g in range(hch)], axis=0)
        parts = []
        for st in range(2):
            for a in range(n_adapt):
                parts.append(jnp.where(ids == a, mids[st * rank:(st + 1) * rank], 0.0).astype(BF16))
        lora = mm(jnp.concatenate(parts, axis=0), btg[...], 0, 1)
        r = pl.ds(y_rows(p, chip, core, 0), rows)
        xo[p] = xv[r, y_cols(chip)].astype(F32) + scale * lora

    def finish_part(p, u):
        if (p, 2, 0) not in met:
            met.add((p, 2, 0))
            d2d(p, chip).wait_recv()
        tot = buf[p, chip, core, sub(u)].astype(F32) + drecv[p, chip, sub(u)].astype(F32)
        for way in range(2):
            ring_copy(p, way, hch - 1 - way, u).wait_recv()
            tot = tot + ring[p, way, hch - 1 - way, sub(u)].astype(F32)
        y_slot(p, chip, core, u)[...] = (xo[p, sub(u)] + tot).astype(BF16)
        ag_ring(p, 0, 0, u).start()
        ag_ring(p, 1, 0, u).start()
        ag_d2d(p, 0, u).start()

    def bt_forward():
        drain_recv(btg.at[pl.ds(0, wide)], bt_r.at[0])
        bt_fwd.start()

    def bt_arrived():
        bt_d2d.wait_recv()
        bt_fwd.wait_recv()

    def rank_sends_done():
        drain_send(gm.at[0, pl.ds(0, chips - 1)], mf_s.at[0])
        drain_send(gm.at[0, pl.ds(0, chips - 1)], mid_s.at[0])
        for p in range(PASSES):
            drain_send(gm.at[p, pl.ds(0, chips)], md_s.at[p])
        drain_send(btg.at[pl.ds(0, 3 * wide)], bt_s.at[0])

    def sum_sends_done(p):
        drain_send(drecv.at[p], dd_s.at[p])
        drain_send(midx.at[p, pl.ds(0, hch - 1)], mg_s.at[p])
        drain_send(midx.at[p], mx_s.at[p])
        mid_part(p).wait_send()
        drain_send(drecv.at[p, pl.ds(0, chips - 1)], rg_s.at[p])

    def y_sends_done(p):
        drain_send(drecv.at[p, pl.ds(0, chips - 1)], ag_s.at[p])
        drain_send(drecv.at[p], ad_s.at[p])

    def y_arrived(p):
        drain_recv(drecv.at[p], ad_r.at[p])

    def ring_step(p, s):
        for u in range(SUBS):
            for way in range(2):
                if s < hch - way:
                    ring_part(p, way, s, u)

    def ag_step(p, s):
        for u in range(SUBS):
            for way in range(2):
                if s < hch - way:
                    ag_part(p, way, s, u)

    def finish_y(p):
        for u in range(SUBS):
            finish_part(p, u)

    w1_ld.wait()
    base_qkv(0)
    bt_ld.wait()
    bt_out(0).start()
    bt_d2d.start()
    w2_ld.wait()
    base_gu(0)
    base_qkv(1)
    mid_forward()
    mid_service(1, 0)
    bt_out(1).start()
    for cp in [cos_ld, sin_ld] + late:
        cp.wait()
    attend(0)
    gated(0)
    mid_service(1, 1)
    groups(0, 0, 2)
    groups(0, 2, 4)
    mid_service(1, 2)
    ring_step(0, 0)
    mid_scatter(0)
    base_gu(1)
    mid_service(1, 3)
    bt_forward()
    attend(1)
    ring_step(0, 1)
    gated(1)
    mid_gather(0)
    groups(1, 0, 2)
    ring_step(0, 2)
    groups(1, 2, 4)
    ring_step(1, 0)
    mid_scatter(1)
    bt_arrived()
    lora_out(0)
    ring_step(0, 3)
    ring_step(1, 1)
    mid_gather(1)
    finish_y(0)
    ring_step(1, 2)
    ag_step(0, 0)
    ring_step(1, 3)
    lora_out(1)
    ag_step(0, 1)
    finish_y(1)
    ag_step(0, 2)
    ag_step(1, 0)
    ag_step(0, 3)
    ag_step(1, 1)
    ag_step(1, 2)
    ag_step(1, 3)
    rank_sends_done()
    for p in range(PASSES):
        sum_sends_done(p)
        y_arrived(p)
        y_sends_done(p)


def solution(mesh):
    n = mesh.shape['tensor']
    batch_spec = P('data', None, None)
    head_cols = P(None, 'tensor', None)
    head_rows = P('tensor', None, None)
    ff_cols = P(None, 'tensor')
    ff_rows = P('tensor', None)
    last_split = P(None, None, 'tensor')
    b_heads = P(None, None, 'tensor', None)
    a_heads = P(None, 'tensor', None, None)
    in_specs = (batch_spec, P('data'), P(None), head_cols, head_cols, head_cols, head_rows, ff_cols, ff_cols, ff_rows, last_split, b_heads, last_split, b_heads, last_split, b_heads, a_heads, last_split, last_split, last_split, last_split, last_split, head_cols, last_split)

    def local_layer(x_blk, adapter_ids, norm_gain, w_query, w_key, w_value, w_out, w_gate, w_up, w_down, a_query, b_query, a_key, b_key, a_value, b_value, a_out, b_out, a_gate, b_gate, a_up, b_up, a_down, b_down):
        seqs, seq, d_model = x_blk.shape
        tokens = seqs * seq
        n_adapt, _, rank = a_down.shape
        heads, head = w_query.shape[1:]
        wide = heads * head
        ff = w_gate.shape[1]
        chips = n // 2
        half = tokens // PASSES
        rows = half // 4
        cols = d_model // (chips // 2)
        mrows = 2 * rank // (chips // 2)
        share = rank // n

        hd = head // 2
        inv_freq = ROPE_BASE ** (-np.arange(hd, dtype=np.float32) / np.float32(hd))
        ang = inv_freq[:, None] * np.arange(seq, dtype=np.float32)[None, :]
        ang = np.tile(ang.astype(np.float32), (1, half // seq))
        cos_t, sin_t = jnp.asarray(np.cos(ang), F32), jnp.asarray(np.sin(ang), F32)

        def wt(w):
            return w.transpose(1, 2, 0).reshape(wide, d_model)

        def at(a):
            return a.transpose(0, 2, 1).reshape(n_adapt * share, d_model)

        def bt(b):
            return b.transpose(0, 2, 3, 1).reshape(n_adapt, wide, rank)

        args = (x_blk.reshape(tokens, d_model), adapter_ids, norm_gain.reshape(d_model // 128, 128), cos_t, sin_t,
                wt(w_query), wt(w_key), wt(w_value), w_out.reshape(wide, d_model), w_gate, w_up, w_down,
                at(a_query), at(a_key), at(a_value), at(a_gate), at(a_up),
                bt(b_query), bt(b_key), bt(b_value), b_gate.reshape(n_adapt * rank, ff), b_up.reshape(n_adapt * rank, ff),
                a_out.reshape(n_adapt, wide, rank), a_down, b_out.transpose(0, 2, 1), b_down.transpose(0, 2, 1))
        hbm = pl.BlockSpec(memory_space=pl.ANY)
        vmem = pl.BlockSpec(memory_space=pltpu.VMEM)
        dma = pltpu.SemaphoreType.DMA
        cfg = (n, tokens, seq, n_adapt, rank, heads, head, ff)
        scratch = [
            pltpu.SMEM((seqs,), jnp.int32),
            pltpu.VMEM((1, tokens), jnp.int32),
            pltpu.VMEM((d_model // 128, 128), F32),
            pltpu.VMEM((1, d_model), F32),
            pltpu.VMEM((hd, half), F32),
            pltpu.VMEM((hd, half), F32),
            pltpu.VMEM((tokens, d_model), BF16),
            pltpu.VMEM((tokens, d_model), BF16),
            pltpu.VMEM((5 * n_adapt * share, d_model), BF16),
            pltpu.VMEM((3 * wide, d_model), BF16),
            pltpu.VMEM((d_model, 2 * ff), BF16),
            pltpu.VMEM((3 * wide, n_adapt * rank), BF16),
            pltpu.VMEM((n_adapt * rank, 2 * ff), BF16),
            pltpu.VMEM((wide, d_model), BF16),
            pltpu.VMEM((ff, d_model), BF16),
            pltpu.VMEM((wide, n_adapt * rank), BF16),
            pltpu.VMEM((ff, n_adapt * rank), BF16),
            pltpu.VMEM((4 * wide, 2 * n_adapt * rank), BF16),
            pltpu.VMEM((3 * wide, tokens), F32),
            pltpu.VMEM((tokens, 2 * ff), F32),
            pltpu.VMEM((PASSES, n, 10 * share, half // 2), BF16),
            pltpu.VMEM((n_adapt * rank, half), BF16),
            pltpu.VMEM((3 * wide, half), BF16),
            pltpu.VMEM((wide, tokens), BF16),
            pltpu.VMEM((tokens, ff), BF16),
            pltpu.VMEM((PASSES, 2, 2, 2 * rank, rows), BF16),
            pltpu.VMEM((PASSES, 2, 2 * rank, rows), BF16),
            pltpu.VMEM((PASSES, chips - 1, mrows, rows), BF16),
            pltpu.VMEM((PASSES, chips, 2, rows, cols), BF16),
            pltpu.VMEM((PASSES, chips, rows, cols), BF16),
            pltpu.VMEM((PASSES, 2, chips // 2, rows, cols), BF16),
            pltpu.VMEM((PASSES, chips // 2, mrows, rows), BF16),
            pltpu.VMEM((PASSES, rows, cols), F32),
            dma((18,)), dma((1,)), dma((1,)),
            dma((1,)), dma((2, 4)), dma((PASSES,)), dma((PASSES,)),
            dma((1,)), dma((3,)), dma((PASSES,)), dma((PASSES, chips)),
            dma((PASSES,)), dma((PASSES, 2, 4, SUBS)),
            dma((PASSES,)), dma((PASSES,)), dma((PASSES,)), dma((PASSES,)),
            dma((PASSES,)), dma((PASSES,)),
            dma((PASSES,)), dma((PASSES, 2, 4, SUBS)), dma((PASSES,)), dma((PASSES,)),
        ]
        y = pl.pallas_call(
            functools.partial(layer_kernel, cfg),
            out_shape=pltpu.VMEM((tokens, d_model), BF16),
            in_specs=[hbm] * 26,
            out_specs=vmem,
            scratch_shapes=scratch,
            compiler_params=pltpu.CompilerParams(collective_id=0, has_side_effects=True,
                                                 vmem_limit_bytes=59_000_000),
        )(*args)
        return y.reshape(x_blk.shape)

    return jax.shard_map(local_layer, mesh=mesh, in_specs=in_specs, out_specs=batch_spec, check_vma=False)
```
